128 devices in a mesh: plane: 8 (over z_hi, x), tile: 16 (over z_lo, y, core).
Axes of the slice: x: 4, y: 4, z: 4 (z_hi: 2, z_lo: 2; z = z_hi * 2 + z_lo), core: 2. Of those that a mesh axis runs over, the one named last changes fastest.
Arguments:
- visibility: float32 [2, 262144], P(None, ('plane', 'tile')), may hold values from -6 to 6
- target: int32 [262144, 1], P(('plane', 'tile')), may hold values from 0 to 127; in each aligned block of 2048 rows (0 to 2047, 2048 to 4095, ...) at most 32 rows name the same one
- offset: int32 [262144], P(('plane', 'tile')), may hold values from 0 to 1048575
- taps: float32 [8], replicated, may hold values from 0.1 to 1
- w_plane: float32 [8], P('plane'), may hold values from -300 to 300
Outputs:
- dirty_image: float32 [4096, 4096], P('plane', 'tile')
The draws below stay inside these ranges and needn't reach their ends.
Inputs may be any that keep to these rules, and one draw needn't show every extreme that they name: `target`: among the rows of one device no value occurs more than 32 times, and some value occurs exactly 32 times.
All inputs are finite; a program needn't handle non-finite values.
Results may differ from the reference program's by a relative error of at most 0.0042.
Values sent between devices are 32-bit elements; how exact they have to be, the bound alone decides.
A program may use at most 128 MiB of HBM per device.

```python
import math
import jax
import jax.numpy as jnp
import numpy as np
from jax import lax

G = 4096
KS = 8
VIS_DEV = 2048
PLANES = 8
ROWS = 256
CAP = 32
VIS_ALL = 262144
N_PLANE = 8
N_TILE = 16


def plant(entries, key, smallest, largest):
    spot = [jax.random.randint(jax.random.fold_in(key, axis), (), 0, length) for axis, length in enumerate(entries.shape)]
    main_axis = entries.shape.index(max(entries.shape))
    neighbour = spot[:main_axis] + [(spot[main_axis] + 1) % entries.shape[main_axis]] + spot[main_axis + 1:]
    return entries.at[tuple(spot)].set(smallest).at[tuple(neighbour)].set(largest)


def shard_levels(own_key, shape, pieces, low, largest):
    level = 1.0
    for dim, parts in pieces:
        draws = jax.random.uniform(jax.random.fold_in(jax.random.fold_in(own_key, 6), dim), (parts,), jnp.float32, low / len(pieces), largest / len(pieces))
        level = level * jnp.repeat(jnp.exp(draws), shape[dim] // parts).reshape((-1,) + (1,) * (len(shape) - 1 - dim))
    return level


def deal_out(key, own, number, rows, count, top, reach, lean):
    sequence = jax.random.permutation(key, count)
    packed, common = load_shares(count, rows * top, reach, lean, True), load_shares(count, rows * top, reach, lean, False)
    places = jnp.arange(count)

    def named(sizes, rotation):
        used = int((sizes > 0).sum())
        fixed = max(1, used // 4)
        shifted = fixed + (places - fixed + rotation * (used - fixed)) % max(1, count - fixed)
        return jnp.zeros((count,), jnp.int32).at[sequence[jnp.where(places < fixed, places, shifted)]].set(jnp.asarray(sizes, jnp.int32))

    sizes = jnp.where(number % 4 == 0, named(packed, number // 4), named(common, number - number // 4 - 1))
    mixed = jax.random.permutation(jax.random.fold_in(own, 3), count)
    donor, receiver = mixed[0:count // 2 * 2:2], mixed[1:count // 2 * 2:2]
    slack = jnp.minimum(sizes[donor] - 1, reach - sizes[receiver]) // 2
    slack = jnp.where((donor == sequence[0]) | (receiver == sequence[0]) | (sizes[receiver] == 0), 0, jnp.maximum(slack, 0))
    shifted = jax.random.randint(jax.random.fold_in(own, 4), (count // 2,), 0, 1 << 20) % (slack + 1)
    sizes = sizes.at[donor].add(-shifted).at[receiver].add(shifted)
    members = jnp.searchsorted(jnp.cumsum(sizes), jnp.arange(rows * top), side="right").astype(jnp.int32)
    grid = members.reshape(top, rows).T
    grid = grid[jax.random.permutation(jax.random.fold_in(own, 1), rows)]
    rotation = jax.random.randint(jax.random.fold_in(own, 2), (rows, 1), 0, top)
    return jnp.take_along_axis(grid, (jnp.arange(top)[None, :] + rotation) % top, axis=1)


def load_shares(number_of, total, limit, skew, full):
    weights = [(1 << 20) // math.isqrt(grade ** skew) + 1 for grade in range(1, number_of + 1)]
    largest = limit if full else min(limit, max(-(-total // number_of), total * weights[0] // sum(weights)))
    least = 1 if total - largest >= number_of - 1 else 0
    holding, spare = [largest] + [least] * (number_of - 1), total - largest - least * (number_of - 1)
    while spare > 0:
        free = [i for i in range(1, number_of) if holding[i] < largest] or [i for i in range(1, number_of) if holding[i] < limit]
        pool, budget = sum([weights[i] for i in free]), spare
        for i in free:
            more = min(limit - holding[i], max(1, budget * weights[i] // pool), spare)
            holding[i] = holding[i] + more
            spare = spare - more
    return np.array(holding)


def gaussian(rng, shape, deviation, most, shards=(), kind=jnp.bfloat16):
    result = deviation * jax.random.normal(rng, shape, jnp.float32)
    if shards:
        result = result * shard_levels(rng, shape, shards, -0.22, 0.18)
    return jnp.clip(result, -most, most).astype(kind)


def setup_inputs(seed: int = 0) -> dict:
    keys = jax.random.split(jax.random.key(seed), 6)
    visibility = gaussian(keys[0], (2, VIS_ALL), 1.0, 6.0, ((1, 128),), jnp.float32)
    target_keys = jax.random.split(jax.random.fold_in(keys[1], 1), VIS_ALL // VIS_DEV)
    target_turns = jax.random.permutation(jax.random.fold_in(keys[1], 3), VIS_ALL // VIS_DEV)
    target = jax.vmap(lambda own, number: deal_out(jax.random.fold_in(keys[1], 2), own, number, VIS_DEV, N_PLANE * N_TILE, 1, CAP, 2))(target_keys, target_turns).reshape((VIS_ALL, 1))
    offset = plant(jax.random.randint(keys[2], (VIS_ALL,), 0, ROWS * G), jax.random.fold_in(keys[2], 1), 0, (ROWS * G) - 1).astype(jnp.int32)
    taps = jnp.clip(jnp.exp(jax.random.uniform(keys[3], (KS,), jnp.float32, math.log(0.1), math.log(1.0))), 0.1, 1.0)
    w_plane = jnp.clip(jax.random.uniform(keys[4], (PLANES,), jnp.float32, -300.0, 300.0) * shard_levels(keys[4], (PLANES,), ((0, 8),), -0.4, 0.0), -300.0, 300.0)
    return dict(visibility=visibility, target=target, offset=offset, taps=taps, w_plane=w_plane)


def direction(index, length):
    return ((index + length // 2) % length - length // 2).astype(jnp.float32) * (0.5 / length)

def reference(visibility, target, offset, taps, w_plane):
    destination = target[:, 0]
    plane_of = destination // N_TILE
    tile_of = destination % N_TILE
    grid_row = tile_of * (G // N_TILE) + offset // G
    grid_col = offset % G
    kernel_len = taps.shape[0]
    count = visibility.shape[1]
    weight_re = lax.optimization_barrier((taps[None, :] * visibility[0][:, None]).astype(jnp.bfloat16)).astype(jnp.float32)
    weight_im = lax.optimization_barrier((taps[None, :] * visibility[1][:, None]).astype(jnp.bfloat16)).astype(jnp.float32)
    taps_round = lax.optimization_barrier(taps.astype(jnp.bfloat16)).astype(jnp.float32)
    shifts = jnp.arange(kernel_len, dtype=jnp.int32)
    row_index = (grid_row[:, None] + shifts[None, :]) % G
    col_index = (grid_col[:, None] + shifts[None, :]) % G
    row_full = jnp.broadcast_to(row_index[:, :, None], (count, kernel_len, kernel_len))
    col_full = jnp.broadcast_to(col_index[:, None, :], (count, kernel_len, kernel_len))
    lines = jnp.arange(G, dtype=jnp.int32)
    cosines = direction(lines, G)
    n_minus = jnp.sqrt(1.0 - cosines[:, None] * cosines[:, None] - cosines[None, :] * cosines[None, :]) - 1.0
    image = jnp.zeros((G, G), jnp.float32)
    for plane in range(N_PLANE):
        mask = (plane_of == plane).astype(jnp.float32)
        value_re = (weight_re * mask[:, None])[:, :, None] * taps_round[None, None, :]
        value_im = (weight_im * mask[:, None])[:, :, None] * taps_round[None, None, :]
        grid_re = jnp.zeros((G, G), jnp.float32).at[row_full, col_full].add(value_re)
        grid_im = jnp.zeros((G, G), jnp.float32).at[row_full, col_full].add(value_im)
        transformed = jnp.fft.ifft2(grid_re + 1j * grid_im) * (G * G)
        phase = 2.0 * math.pi * w_plane[plane] * n_minus
        image = image + (jnp.cos(phase) * jnp.real(transformed) - jnp.sin(phase) * jnp.imag(transformed))
    return image * (1.0 / math.sqrt(VIS_ALL))
```

```python
import math

import jax
import jax.numpy as jnp
import numpy as np
from jax import lax
from jax.experimental import pallas as pl
from jax.experimental.pallas import tpu as pltpu
from jax.sharding import PartitionSpec as P


G = 4096
KS = 8
MESH = pl.DeviceIdType.MESH
F32 = jnp.float32
BF16 = jnp.bfloat16
NT = (((1,), (1,)), ((), ()))

SIN = (3.1415927410125732, -5.167710304260254, 2.550077438354492, -0.598291277885437, 0.07765766233205795)
COS = (0.9999999403953552, -4.934792995452881, 4.058411121368408, -1.331876516342163, 0.21968960762023926)


def poly(coefs, g):
    out = g * coefs[-1] + coefs[-2]
    for c in coefs[-3::-1]:
        out = out * g + c
    return out


def cos_sin(cycles):
    f = cycles - jnp.floor(cycles + 0.5)
    g = f * f
    s = f * poly(SIN, g)
    c = poly(COS, g)
    s2 = s + s
    return 1.0 - s2 * s, s2 * c


def rotated(re, im, c, s):
    return re * c - im * s, re * s + im * c


def sort_kernel(vis_ref, tgt_ref, off_ref, out_ref):
    count = tgt_ref.shape[1]
    blk = 256
    ii = lax.broadcasted_iota(jnp.int32, (blk, blk), 0)
    jj = lax.broadcasted_iota(jnp.int32, (blk, blk), 1)
    tri = jnp.where(ii < jj, 1.0, 0.0).astype(BF16)
    rows = lax.broadcasted_iota(jnp.int32, (128, blk), 0)
    ranks = lax.broadcasted_iota(jnp.int32, (32, blk), 0).astype(F32)
    carry = jnp.zeros((128, 1), F32)
    acc = jnp.zeros((128, 128), F32)
    for b in range(count // blk):
        sl = slice(b * blk, (b + 1) * blk)
        one = jnp.where(rows == tgt_ref[:, sl], 1.0, 0.0)
        oneb = one.astype(BF16)
        before = jnp.dot(oneb, tri, preferred_element_type=F32)
        rank = jnp.sum(one * (before + carry), axis=0, keepdims=True)
        carry = carry + jnp.sum(one, axis=1, keepdims=True)
        hit = ranks == rank
        off = off_ref[:, sl]
        parts = [((off >> 12) << 12).astype(F32), (((off >> 4) & 255) << 4).astype(F32), (off & 15).astype(F32)]
        left = [vis_ref[0:1, sl], vis_ref[1:2, sl]]
        for k in range(3):
            cols = []
            for v in range(2):
                top = left[v].astype(BF16).astype(F32)
                left[v] = left[v] - top
                cols.append(jnp.where(hit, top, 0.0))
            cols.append(jnp.where(hit, parts[k], 0.0))
            cols.append(jnp.zeros((32, blk), F32))
            table = jnp.concatenate(cols, axis=0).astype(BF16)
            acc = acc + lax.dot_general(oneb, table, NT, preferred_element_type=F32)
    out_ref[...] = acc


def sort_call(vis, tgt, off):
    return pl.pallas_call(
        sort_kernel,
        out_shape=jax.ShapeDtypeStruct((128, 128), F32),
        in_specs=[pl.BlockSpec(memory_space=pltpu.VMEM)] * 3,
        out_specs=pl.BlockSpec(memory_space=pltpu.VMEM),
        name="sortvis",
    )(vis, tgt, off)


def place():
    p = lax.axis_index("plane")
    t = lax.axis_index("tile")
    zh, x = p // 4, p % 4
    zl, y, core = t // 8, (t // 2) % 4, t % 2
    return zh, x, zl, y, core


def exchange_kernel(s_ref, w_ref, ga_ref, wo_ref, ra, sa, qa, sy, qy, sz, qz, sc, qc, sw, qw):
    zh, x, zl, y, core = place()
    z = zh * 2 + zl
    p, t = zh * 4 + x, zl * 8 + y * 2 + core

    def at_x(d):
        return {"plane": zh * 4 + (x + d) % 4, "tile": t}

    def at_y(d):
        return {"plane": p, "tile": zl * 8 + ((y + d) % 4) * 2 + core}

    def at_z(d):
        zz = (z + d) % 4
        return {"plane": (zz // 2) * 4 + x, "tile": (zz % 2) * 8 + y * 2 + core}

    partner = {"plane": p, "tile": zl * 8 + y * 2 + (1 - core)}

    barrier = pltpu.get_barrier_semaphore()
    for d in (1, 2, 3):
        for at in (at_x, at_y, at_z):
            pl.semaphore_signal(barrier, inc=1, device_id=at(d), device_id_type=MESH)
    pl.semaphore_signal(barrier, inc=1, device_id=partner, device_id_type=MESH)
    pl.semaphore_wait(barrier, 10)

    def copy(src, dst, send, recv, device):
        c = pltpu.make_async_remote_copy(
            src_ref=src, dst_ref=dst, send_sem=send, recv_sem=recv, device_id=device, device_id_type=MESH
        )
        c.start()
        return c

    first = [copy(s_ref.at[:, (x + d) % 4], ra.at[x], sa.at[d - 1], qa.at[d - 1], at_x(d)) for d in (1, 2, 3)]
    wcopy = copy(w_ref, wo_ref.at[zh], sw, qw, at_z(2))
    wo_ref[zh] = w_ref[...]
    ra[x] = s_ref[:, x]
    for c in first:
        c.wait()
    got = [ra[s].reshape(32, 128) for s in range(4)]
    group = lax.broadcasted_iota(jnp.int32, (32, 128), 1) // 32
    for k in range(3):
        row = jnp.zeros((32, 128), F32)
        for s in range(4):
            shift = (32 * (s - k)) % 128
            moved = pltpu.roll(got[s], shift, 1) if shift else got[s]
            row = jnp.where(group == s, moved, row)
        ga_ref[z, y, core, 0, k] = row[:16]
        ga_ref[z, y, core, 1, k] = row[16:]
    mine = ga_ref.at[z, y, core]
    one_y = [copy(mine.at[0], mine.at[0], sy.at[0, d - 1], qy.at[0, d - 1], at_y(d)) for d in (1, 3, 2)]
    one_z = [copy(mine.at[1], mine.at[1], sz.at[0, d - 1], qz.at[0, d - 1], at_z(d)) for d in (1, 3, 2)]
    for c in one_y:
        c.wait()
    part = ga_ref.at[z, :, core, 0]
    two_z = [copy(part, part, sz.at[1, d - 1], qz.at[1, d - 1], at_z(d)) for d in (1, 3, 2)]
    for c in one_z:
        c.wait()
    part = ga_ref.at[:, y, core, 1]
    two_y = [copy(part, part, sy.at[1, d - 1], qy.at[1, d - 1], at_y(d)) for d in (1, 3, 2)]
    for c in two_z:
        c.wait()
    part = ga_ref.at[:, :, core, 0]
    last = [copy(part, part, sc.at[0], qc.at[0], partner)]
    for c in two_y:
        c.wait()
    part = ga_ref.at[:, :, core, 1]
    last.append(copy(part, part, sc.at[1], qc.at[1], partner))
    wcopy.wait()
    for c in last:
        c.wait()


def exchange_call(s, w):
    dma = pltpu.SemaphoreType.DMA
    return pl.pallas_call(
        exchange_kernel,
        out_shape=(jax.ShapeDtypeStruct((4, 4, 2, 2, 3, 16, 128), F32), jax.ShapeDtypeStruct((2, 8, 128), F32)),
        in_specs=[pl.BlockSpec(memory_space=pltpu.VMEM)] * 2,
        out_specs=(pl.BlockSpec(memory_space=pltpu.VMEM),) * 2,
        scratch_shapes=[
            pltpu.VMEM((4, 2, 16, 128), F32),
            dma((3,)),
            dma((3,)),
            dma((2, 3)),
            dma((2, 3)),
            dma((2, 3)),
            dma((2, 3)),
            dma((2,)),
            dma((2,)),
            dma,
            dma,
        ],
        compiler_params=pltpu.CompilerParams(collective_id=0, has_side_effects=True),
        name="exchangevis",
    )(s, w)


def dft(re, im):
    n = len(re)
    if n == 1:
        return re, im
    er, ei = dft(re[0::2], im[0::2])
    dr, di = dft(re[1::2], im[1::2])
    h = n // 2
    out_r, out_i = [None] * n, [None] * n
    for k in range(h):
        if k == 0:
            tr, ti = dr[k], di[k]
        elif 4 * k == n:
            tr, ti = -di[k], dr[k]
        elif 8 * k == n:
            q = math.sqrt(0.5)
            tr, ti = (dr[k] - di[k]) * q, (dr[k] + di[k]) * q
        elif 8 * k == 3 * n:
            q = math.sqrt(0.5)
            tr, ti = (dr[k] + di[k]) * -q, (dr[k] - di[k]) * q
        else:
            c, s = math.cos(2 * math.pi * k / n), math.sin(2 * math.pi * k / n)
            tr, ti = dr[k] * c - di[k] * s, dr[k] * s + di[k] * c
        out_r[k], out_i[k] = er[k] + tr, ei[k] + ti
        out_r[k + h], out_i[k + h] = er[k] - tr, ei[k] - ti
    return out_r, out_i


def grid_kernel(mb_ref, ga_ref, tw_ref, out_ref, hs, xs, ts, rs, iota, *bufs):
    tabs, hots = bufs[:4], bufs[4:]
    mb = mb_ref[0]
    iota[...] = lax.broadcasted_iota(jnp.int32, (256, 128), 0).astype(F32).astype(BF16)

    def fill(zh, band, g):
        start = g * 8 * 96 + zh * 48 + band
        re = ga_ref[pl.ds(start, 8, stride=96), :]
        im = ga_ref[pl.ds(start + 16, 8, stride=96), :]
        off = ga_ref[pl.ds(start + 32, 8, stride=96), :]
        row = jnp.floor(off * (1.0 / G))
        col = off - row * G
        cb, sb = cos_sin(col * mb * (1.0 / G))
        c1, s1 = cos_sin(col * (1.0 / G))
        c8, s8 = cos_sin(col * (8.0 / G))
        re, im = rotated(re, im, cb, sb)
        for s in range(8):
            nr, ni = rotated(re, im, c8, s8)
            xs[g, 0, s * 8 : s * 8 + 8] = re
            xs[g, 1, s * 8 : s * 8 + 8] = im
            xs[g, 2, s * 8 : s * 8 + 8] = nr
            xs[g, 3, s * 8 : s * 8 + 8] = ni
            if s < 7:
                re, im = rotated(re, im, c1, s1)
        ts[g] = c8 + c8
        rs[g] = row
        tab, hot = tabs[g], hots[g]
        for dev in range(8):
            lanes = slice(dev * 128, dev * 128 + 128)
            t = jnp.broadcast_to(ts[g, dev : dev + 1, :], (8, 128))
            for v in range(2):
                a = xs[g, v, pl.ds(dev, 8, stride=8), :]
                b = xs[g, 2 + v, pl.ds(dev, 8, stride=8), :]
                for k in range(0, 16, 2):
                    tab[v * 128 + k * 8 : v * 128 + k * 8 + 16, lanes] = jnp.concatenate([a, b], axis=0).astype(BF16)
                    if k < 14:
                        a = t * b - a
                        b = t * a - b
            r = jnp.broadcast_to(rs[g, dev : dev + 1, :], (16, 128)).astype(BF16)
            for j in range(16):
                hot[j * 16 : j * 16 + 16, lanes] = jnp.where(
                    iota[j * 16 : j * 16 + 16] == r, jnp.ones((), BF16), jnp.zeros((), BF16)
                )

    def product(g):
        return lax.dot_general(tabs[g][...], hots[g][...], NT, preferred_element_type=F32)

    def plane(zh, _):
        def bands(band, _):
            for g in range(4):
                fill(zh, band, g)
            acc = product(0)
            for g in range(1, 4):
                acc = acc + product(g)
            hs[band] = acc
            return 0

        lax.fori_loop(0, 16, bands, 0)

        def strip(i, _):
            m = pl.multiple_of(i * 16, 16)
            for h in range(2):
                lanes = slice(h * 128, h * 128 + 128)
                re = [hs[b, pl.ds(m, 16), lanes] for b in range(16)]
                im = [hs[b, pl.ds(m + 128, 16), lanes] for b in range(16)]
                re, im = dft(re, im)
                for q in range(16):
                    a, b = re[q], im[q]
                    if q:
                        a, b = rotated(a, b, tw_ref[0, q : q + 1, lanes], tw_ref[1, q : q + 1, lanes])
                    out_ref[zh, q, pl.ds(m, 16), lanes] = a.astype(BF16)
                    out_ref[zh, q, pl.ds(m + 128, 16), lanes] = b.astype(BF16)
            return 0

        lax.fori_loop(0, 8, strip, 0)
        return 0

    lax.fori_loop(0, 2, plane, 0)


def grid_call(mb, ga, tw):
    vmem = pl.BlockSpec(memory_space=pltpu.VMEM)
    return pl.pallas_call(
        grid_kernel,
        out_shape=jax.ShapeDtypeStruct((2, 16, 256, 256), BF16),
        in_specs=[pl.BlockSpec(memory_space=pltpu.SMEM), vmem, vmem],
        out_specs=vmem,
        scratch_shapes=[
            pltpu.VMEM((16, 256, 256), F32),
            pltpu.VMEM((4, 4, 64, 128), F32),
            pltpu.VMEM((4, 8, 128), F32),
            pltpu.VMEM((4, 8, 128), F32),
            pltpu.VMEM((256, 128), BF16),
        ]
        + [pltpu.VMEM((256, 1024), BF16)] * 8,
        compiler_params=pltpu.CompilerParams(vmem_limit_bytes=32 << 20),
        name="gridvis",
    )(mb, ga, tw)


def image_kernel(ab_ref, hp_ref, w_ref, dm_ref, out_ref, sr, si, pb, r1, fw, rc, rd, zb, zr, *sems):
    s1, q1, sf, qf, sd, qd, sz, qz = sems
    zh, x, zl, y, core = place()
    t = zl * 8 + y * 2 + core
    xp, xm = (x + 1) % 4, (x + 3) % 4
    right, left = {"plane": zh * 4 + xp, "tile": t}, {"plane": zh * 4 + xm, "tile": t}
    across = {"plane": (1 - zh) * 4 + x, "tile": t}

    barrier = pltpu.get_barrier_semaphore()
    for dev in (right, left, across):
        pl.semaphore_signal(barrier, inc=1, device_id=dev, device_id_type=MESH)

    l0 = lax.broadcasted_iota(jnp.int32, (256, 128), 0)
    lane = lax.broadcasted_iota(jnp.int32, (256, 128), 1)
    ec, es = cos_sin((l0 * 16 + lane).astype(F32) * (1.0 / G))
    ar, ai = jnp.full((256, 128), ab_ref[0, KS - 1]), jnp.zeros((256, 128), F32)
    for j in range(KS - 2, -1, -1):
        ar, ai = rotated(ar, ai, ec, es)
        ar = ar + ab_ref[0, j]
    sr[...] = ar
    si[...] = ai
    m = t * 256 + zh * 128 + lax.broadcasted_iota(jnp.int32, (8, 128), 1)
    ec, es = cos_sin(m.astype(F32) * (1.0 / G))
    tr, ti = jnp.full((8, 128), ab_ref[1, KS - 1]), jnp.zeros((8, 128), F32)
    for j in range(KS - 2, -1, -1):
        tr, ti = rotated(tr, ti, ec, es)
        tr = tr + ab_ref[1, j]
    tr, ti = tr[0:1] * (1.0 / 512.0), ti[0:1] * (1.0 / 512.0)
    ym = jnp.where(m >= G // 2, m - G, m).astype(F32)[0:1] * (0.5 / G)
    ysq = ym * ym
    ws = [w_ref[q, 0:1, :] for q in range(2)]
    row = lax.broadcasted_iota(jnp.int32, (64, 128), 0)

    pl.semaphore_wait(barrier, 3)

    def copy(src, dst, send, recv, device):
        return pltpu.make_async_remote_copy(
            src_ref=src, dst_ref=dst, send_sem=send, recv_sem=recv, device_id=device, device_id_type=MESH
        )

    def step_one(i):
        xo = (x + 2) % 4
        return (
            copy(pb.at[i, 0, xo], r1.at[i, 0], s1.at[i, 0], q1.at[i, 0], right),
            copy(pb.at[i, 1, xo], r1.at[i, 1], s1.at[i, 1], q1.at[i, 1], left),
        )

    def direct(i):
        return (
            copy(pb.at[i, 0, xm], rd.at[i, 0], sd.at[i, 0], qd.at[i, 0], left),
            copy(pb.at[i, 1, xp], rd.at[i, 1], sd.at[i, 1], qd.at[i, 1], right),
        )

    def forward(i):
        return (
            copy(fw.at[i, 0], rc.at[i, 0], sf.at[i, 0], qf.at[i, 0], right),
            copy(fw.at[i, 1], rc.at[i, 1], sf.at[i, 1], qf.at[i, 1], left),
        )

    def over(i):
        return copy(zb.at[i], zr.at[i], sz.at[i], qz.at[i], across)

    def compute(i):
        for q in range(4):
            rows = slice(q * 64, q * 64 + 64)
            l = (row + q * 64) * 16 + i
            xl = jnp.where(l >= G // 2, l - G, l).astype(F32) * (0.5 / G)
            rho = xl * xl + ysq
            n = -rho / (1.0 + jnp.sqrt(1.0 - rho))
            zre = zim = None
            for v in range(2):
                hp = hp_ref[v, i]
                pc = lax.dot_general(dm_ref[rows, :], hp, NT, preferred_element_type=F32)
                ps = lax.dot_general(dm_ref[256 + q * 64 : 320 + q * 64, :], hp, NT, preferred_element_type=F32)
                dre = pc[:, :128] - ps[:, 128:]
                dim = ps[:, :128] + pc[:, 128:]
                c, s = cos_sin(ws[v] * n)
                a, b = rotated(dre, dim, c, s)
                zre, zim = (a, b) if zre is None else (zre + a, zim + b)
            a, b = rotated(zre, zim, tr, ti)
            lanes = lax.broadcasted_iota(jnp.int32, (64, 128), 1)
            cs = jnp.sum(jnp.where(lanes == i, sr[rows], 0.0), axis=1, keepdims=True)
            ss = jnp.sum(jnp.where(lanes == i, si[rows], 0.0), axis=1, keepdims=True)
            part = cs * a - ss * b
            for k in range(2):
                pb[i, q // 2, (q % 2) * 2 + k] = part[k * 32 : k * 32 + 32]

    def put(i, half, value):
        out_ref[pl.ds(half * 512 + i, 32, stride=16), :] = value

    lag1, lag2, lag3 = 1, 3, 5

    def turn(i, _):
        @pl.when(i < 16)
        def _():
            compute(i)
            for c in step_one(i) + direct(i):
                c.start()

        @pl.when(jnp.logical_and(i >= lag1, i < 16 + lag1))
        def _():
            j = i - lag1
            for c in step_one(j):
                c.wait_recv()
            fw[j, 0] = r1[j, 0] + pb[j, 0, xp]
            fw[j, 1] = r1[j, 1] + pb[j, 1, xm]
            for c in forward(j):
                c.start()

        @pl.when(jnp.logical_and(i >= lag2, i < 16 + lag2))
        def _():
            j = i - lag2
            for c in forward(j) + direct(j):
                c.wait_recv()
            put(j, zh, pb[j, zh, x] + rc[j, zh] + rd[j, zh])
            zb[j] = pb[j, 1 - zh, x] + rc[j, 1 - zh] + rd[j, 1 - zh]
            over(j).start()

        @pl.when(i >= lag3)
        def _():
            j = i - lag3
            over(j).wait_recv()
            put(j, 1 - zh, zr[j])

        return 0

    lax.fori_loop(0, 16 + lag3, turn, 0)

    def drain(i, _):
        for c in step_one(i) + direct(i) + forward(i) + (over(i),):
            c.wait_send()
        return 0

    lax.fori_loop(0, 16, drain, 0)


def image_call(ab, hp, w, dm):
    dma = pltpu.SemaphoreType.DMA
    vmem = pl.BlockSpec(memory_space=pltpu.VMEM)
    buf = pltpu.VMEM((16, 2, 32, 128), F32)
    half = pltpu.VMEM((16, 32, 128), F32)
    return pl.pallas_call(
        image_kernel,
        out_shape=jax.ShapeDtypeStruct((1024, 128), F32),
        in_specs=[pl.BlockSpec(memory_space=pltpu.SMEM), vmem, vmem, vmem],
        out_specs=vmem,
        scratch_shapes=[pltpu.VMEM((256, 128), F32)] * 2
        + [pltpu.VMEM((16, 2, 4, 32, 128), F32), buf, buf, buf, buf, half, half]
        + [dma((16, 2))] * 6
        + [dma((16,))] * 2,
        compiler_params=pltpu.CompilerParams(collective_id=1, has_side_effects=True, vmem_limit_bytes=32 << 20),
        name="imagesum",
    )(ab, hp, w, dm)


def constants():
    k = np.arange(256)
    a = 2 * np.pi * (np.outer(k, k) % 256) / 256
    dm = np.concatenate([np.cos(a), np.sin(a)], axis=0)
    b = 2 * np.pi * np.outer(np.arange(16), k) / G
    return dm.astype(jnp.bfloat16), np.stack([np.cos(b), np.sin(b)]).astype(np.float32)


def local(visibility, target, offset, taps, w_plane):
    dm, tw = constants()
    count = visibility.shape[1]
    s = sort_call(visibility, target.reshape(1, count), offset.reshape(1, count))
    w = jnp.broadcast_to(w_plane.reshape(1, 1), (8, 128))
    ga, wo = exchange_call(s.reshape(2, 4, 16, 128), w)
    mb = lax.axis_index("tile") * 256 + (lax.axis_index("plane") // 4) * 128
    hp = grid_call(mb.astype(F32).reshape(1), ga.reshape(32 * 96, 128), jnp.asarray(tw))
    ab = jnp.stack([taps, taps.astype(BF16).astype(F32)])
    halves = image_call(ab, hp, wo, jnp.asarray(dm))
    return jnp.concatenate([halves[:512], halves[512:]], axis=1)


def solution(mesh):
    planes, tiles = ("plane",), ("tile",)
    both = planes + tiles
    return jax.shard_map(
        local,
        mesh=mesh,
        in_specs=(P(None, both), P(both, None), P(both), P(), P("plane")),
        out_specs=P("plane", "tile"),
        check_vma=False,
    )
```

```python
import math

import jax
import jax.numpy as jnp
import numpy as np
from jax import lax
from jax.experimental import pallas as pl
from jax.experimental.pallas import tpu as pltpu
from jax.sharding import PartitionSpec as P


G = 4096
KS = 8
MESH = pl.DeviceIdType.MESH
F32 = jnp.float32
BF16 = jnp.bfloat16
NT = (((1,), (1,)), ((), ()))

SIN = (3.1415927410125732, -5.167710304260254, 2.550077438354492, -0.598291277885437, 0.07765766233205795)
COS = (0.9999999403953552, -4.934792995452881, 4.058411121368408, -1.331876516342163, 0.21968960762023926)


def poly(coefs, g):
    out = g * coefs[-1] + coefs[-2]
    for c in coefs[-3::-1]:
        out = out * g + c
    return out


def cos_sin(cycles):
    f = cycles - jnp.floor(cycles + 0.5)
    g = f * f
    s = f * poly(SIN, g)
    c = poly(COS, g)
    s2 = s + s
    return 1.0 - s2 * s, s2 * c


def rotated(re, im, c, s):
    return re * c - im * s, re * s + im * c


def sort_kernel(vis_ref, tgt_ref, off_ref, out_ref):
    count = tgt_ref.shape[1]
    blk = 256
    ii = lax.broadcasted_iota(jnp.int32, (blk, blk), 0)
    jj = lax.broadcasted_iota(jnp.int32, (blk, blk), 1)
    tri = jnp.where(ii < jj, 1.0, 0.0).astype(BF16)
    rows = lax.broadcasted_iota(jnp.int32, (128, blk), 0)
    ranks = lax.broadcasted_iota(jnp.int32, (32, blk), 0).astype(F32)
    carry = jnp.zeros((128, 1), F32)
    acc = jnp.zeros((128, 128), F32)
    for b in range(count // blk):
        sl = slice(b * blk, (b + 1) * blk)
        one = jnp.where(rows == tgt_ref[:, sl], 1.0, 0.0)
        oneb = one.astype(BF16)
        before = jnp.dot(oneb, tri, preferred_element_type=F32)
        rank = jnp.sum(one * (before + carry), axis=0, keepdims=True)
        carry = carry + jnp.sum(one, axis=1, keepdims=True)
        hit = ranks == rank
        off = off_ref[:, sl]
        parts = [((off >> 12) << 12).astype(F32), (((off >> 4) & 255) << 4).astype(F32), (off & 15).astype(F32)]
        left = [vis_ref[0:1, sl], vis_ref[1:2, sl]]
        for k in range(3):
            cols = []
            for v in range(2):
                top = left[v].astype(BF16).astype(F32)
                left[v] = left[v] - top
                cols.append(jnp.where(hit, top, 0.0))
            cols.append(jnp.where(hit, parts[k], 0.0))
            cols.append(jnp.zeros((32, blk), F32))
            table = jnp.concatenate(cols, axis=0).astype(BF16)
            acc = acc + lax.dot_general(oneb, table, NT, preferred_element_type=F32)
    out_ref[...] = acc


def sort_call(vis, tgt, off):
    return pl.pallas_call(
        sort_kernel,
        out_shape=jax.ShapeDtypeStruct((128, 128), F32),
        in_specs=[pl.BlockSpec(memory_space=pltpu.VMEM)] * 3,
        out_specs=pl.BlockSpec(memory_space=pltpu.VMEM),
        name="sortvis",
    )(vis, tgt, off)


def place():
    p = lax.axis_index("plane")
    t = lax.axis_index("tile")
    zh, x = p // 4, p % 4
    zl, y, core = t // 8, (t // 2) % 4, t % 2
    return zh, x, zl, y, core


def exchange_kernel(s_ref, w_ref, ga_ref, wo_ref, ra, sa, qa, sy, qy, sz, qz, sc, qc, sw, qw):
    zh, x, zl, y, core = place()
    z = zh * 2 + zl
    p, t = zh * 4 + x, zl * 8 + y * 2 + core

    def at_x(d):
        return {"plane": zh * 4 + (x + d) % 4, "tile": t}

    def at_y(d):
        return {"plane": p, "tile": zl * 8 + ((y + d) % 4) * 2 + core}

    def at_z(d):
        zz = (z + d) % 4
        return {"plane": (zz // 2) * 4 + x, "tile": (zz % 2) * 8 + y * 2 + core}

    partner = {"plane": p, "tile": zl * 8 + y * 2 + (1 - core)}

    barrier = pltpu.get_barrier_semaphore()
    for d in (1, 2, 3):
        for at in (at_x, at_y, at_z):
            pl.semaphore_signal(barrier, inc=1, device_id=at(d), device_id_type=MESH)
    pl.semaphore_signal(barrier, inc=1, device_id=partner, device_id_type=MESH)
    pl.semaphore_wait(barrier, 10)

    def copy(src, dst, send, recv, device):
        c = pltpu.make_async_remote_copy(
            src_ref=src, dst_ref=dst, send_sem=send, recv_sem=recv, device_id=device, device_id_type=MESH
        )
        c.start()
        return c

    first = [copy(s_ref.at[:, (x + d) % 4], ra.at[x], sa.at[d - 1], qa.at[d - 1], at_x(d)) for d in (1, 2, 3)]
    wcopy = copy(w_ref, wo_ref.at[zh], sw, qw, at_z(2))
    wo_ref[zh] = w_ref[...]
    ra[x] = s_ref[:, x]
    for c in first:
        c.wait()
    got = [ra[s].reshape(32, 128) for s in range(4)]
    group = lax.broadcasted_iota(jnp.int32, (32, 128), 1) // 32
    for k in range(3):
        row = jnp.zeros((32, 128), F32)
        for s in range(4):
            shift = (32 * (s - k)) % 128
            moved = pltpu.roll(got[s], shift, 1) if shift else got[s]
            row = jnp.where(group == s, moved, row)
        ga_ref[z, y, core, 0, k] = row[:16]
        ga_ref[z, y, core, 1, k] = row[16:]
    mine = ga_ref.at[z, y, core]
    one_y = [copy(mine.at[0], mine.at[0], sy.at[0, d - 1], qy.at[0, d - 1], at_y(d)) for d in (1, 3, 2)]
    one_z = [copy(mine.at[1], mine.at[1], sz.at[0, d - 1], qz.at[0, d - 1], at_z(d)) for d in (1, 3, 2)]
    for c in one_y:
        c.wait()
    part = ga_ref.at[z, :, core, 0]
    two_z = [copy(part, part, sz.at[1, d - 1], qz.at[1, d - 1], at_z(d)) for d in (1, 3, 2)]
    for c in one_z:
        c.wait()
    part = ga_ref.at[:, y, core, 1]
    two_y = [copy(part, part, sy.at[1, d - 1], qy.at[1, d - 1], at_y(d)) for d in (1, 3, 2)]
    for c in two_z:
        c.wait()
    part = ga_ref.at[:, :, core, 0]
    last = [copy(part, part, sc.at[0], qc.at[0], partner)]
    for c in two_y:
        c.wait()
    part = ga_ref.at[:, :, core, 1]
    last.append(copy(part, part, sc.at[1], qc.at[1], partner))
    wcopy.wait()
    for c in last:
        c.wait()


def exchange_call(s, w):
    dma = pltpu.SemaphoreType.DMA
    return pl.pallas_call(
        exchange_kernel,
        out_shape=(jax.ShapeDtypeStruct((4, 4, 2, 2, 3, 16, 128), F32), jax.ShapeDtypeStruct((2, 8, 128), F32)),
        in_specs=[pl.BlockSpec(memory_space=pltpu.VMEM)] * 2,
        out_specs=(pl.BlockSpec(memory_space=pltpu.VMEM),) * 2,
        scratch_shapes=[
            pltpu.VMEM((4, 2, 16, 128), F32),
            dma((3,)),
            dma((3,)),
            dma((2, 3)),
            dma((2, 3)),
            dma((2, 3)),
            dma((2, 3)),
            dma((2,)),
            dma((2,)),
            dma,
            dma,
        ],
        compiler_params=pltpu.CompilerParams(collective_id=0, has_side_effects=True),
        name="exchangevis",
    )(s, w)


def dft(re, im):
    n = len(re)
    if n == 1:
        return re, im
    er, ei = dft(re[0::2], im[0::2])
    dr, di = dft(re[1::2], im[1::2])
    h = n // 2
    out_r, out_i = [None] * n, [None] * n
    for k in range(h):
        if k == 0:
            tr, ti = dr[k], di[k]
        elif 4 * k == n:
            tr, ti = -di[k], dr[k]
        elif 8 * k == n:
            q = math.sqrt(0.5)
            tr, ti = (dr[k] - di[k]) * q, (dr[k] + di[k]) * q
        elif 8 * k == 3 * n:
            q = math.sqrt(0.5)
            tr, ti = (dr[k] + di[k]) * -q, (dr[k] - di[k]) * q
        else:
            c, s = math.cos(2 * math.pi * k / n), math.sin(2 * math.pi * k / n)
            tr, ti = dr[k] * c - di[k] * s, dr[k] * s + di[k] * c
        out_r[k], out_i[k] = er[k] + tr, ei[k] + ti
        out_r[k + h], out_i[k + h] = er[k] - tr, ei[k] - ti
    return out_r, out_i


def grid_kernel(mb_ref, ga_ref, tw_ref, out_ref, hs, xs, ts, rs, *bufs):
    tabs, hots = bufs[:4], bufs[4:]
    mb = mb_ref[0]
    sub = lax.broadcasted_iota(jnp.int32, (8, 128), 0).astype(F32)

    def fill(zh, band, g):
        start = g * 8 * 96 + zh * 48 + band
        re = ga_ref[pl.ds(start, 8, stride=96), :]
        im = ga_ref[pl.ds(start + 16, 8, stride=96), :]
        off = ga_ref[pl.ds(start + 32, 8, stride=96), :]
        row = jnp.floor(off * (1.0 / G))
        col = off - row * G
        cb, sb = cos_sin(col * mb * (1.0 / G))
        c1, s1 = cos_sin(col * (1.0 / G))
        c8, s8 = cos_sin(col * (8.0 / G))
        re, im = rotated(re, im, cb, sb)
        for s in range(8):
            nr, ni = rotated(re, im, c8, s8)
            xs[g, 0, s * 8 : s * 8 + 8] = re
            xs[g, 1, s * 8 : s * 8 + 8] = im
            xs[g, 2, s * 8 : s * 8 + 8] = nr
            xs[g, 3, s * 8 : s * 8 + 8] = ni
            if s < 7:
                re, im = rotated(re, im, c1, s1)
        ts[g] = c8 + c8
        rs[g] = row
        tab, hot = tabs[g], hots[g]
        for dev in range(8):
            lanes = slice(dev * 128, dev * 128 + 128)
            t = jnp.broadcast_to(ts[g, dev : dev + 1, :], (8, 128))
            for v in range(2):
                a = xs[g, v, pl.ds(dev, 8, stride=8), :]
                b = xs[g, 2 + v, pl.ds(dev, 8, stride=8), :]
                for k in range(16):
                    tab[v * 128 + k * 8 : v * 128 + k * 8 + 8, lanes] = a
                    a, b = b, t * b - a
            r = jnp.broadcast_to(rs[g, dev : dev + 1, :], (8, 128)) - sub
            for j in range(32):
                hot[j * 8 : j * 8 + 8, lanes] = jnp.where(r == 8.0 * j, 1.0, 0.0)

    def product(g):
        return lax.dot_general(tabs[g][...], hots[g][...], NT, preferred_element_type=F32)

    def plane(zh, _):
        def bands(band, _):
            for g in range(4):
                fill(zh, band, g)
            acc = product(0)
            for g in range(1, 4):
                acc = acc + product(g)
            hs[band] = acc
            return 0

        lax.fori_loop(0, 16, bands, 0)

        def strip(i, _):
            m = pl.multiple_of(i * 16, 16)
            for h in range(2):
                lanes = slice(h * 128, h * 128 + 128)
                re = [hs[b, pl.ds(m, 16), lanes] for b in range(16)]
                im = [hs[b, pl.ds(m + 128, 16), lanes] for b in range(16)]
                re, im = dft(re, im)
                for q in range(16):
                    a, b = re[q], im[q]
                    if q:
                        a, b = rotated(a, b, tw_ref[0, q : q + 1, lanes], tw_ref[1, q : q + 1, lanes])
                    out_ref[zh, q, pl.ds(m, 16), lanes] = a.astype(BF16)
                    out_ref[zh, q, pl.ds(m + 128, 16), lanes] = b.astype(BF16)
            return 0

        lax.fori_loop(0, 8, strip, 0)
        return 0

    lax.fori_loop(0, 2, plane, 0)


def grid_call(mb, ga, tw):
    vmem = pl.BlockSpec(memory_space=pltpu.VMEM)
    return pl.pallas_call(
        grid_kernel,
        out_shape=jax.ShapeDtypeStruct((2, 16, 256, 256), BF16),
        in_specs=[pl.BlockSpec(memory_space=pltpu.SMEM), vmem, vmem],
        out_specs=vmem,
        scratch_shapes=[
            pltpu.VMEM((16, 256, 256), F32),
            pltpu.VMEM((4, 4, 64, 128), F32),
            pltpu.VMEM((4, 8, 128), F32),
            pltpu.VMEM((4, 8, 128), F32),
        ]
        + [pltpu.VMEM((256, 1024), F32)] * 8,
        compiler_params=pltpu.CompilerParams(vmem_limit_bytes=32 << 20),
        name="gridvis",
    )(mb, ga, tw)


def image_kernel(ab_ref, hp_ref, w_ref, dm_ref, out_ref, sr, si, pb, r1, fw, rc, rd, zb, zr, *sems):
    s1, q1, sf, qf, sd, qd, sz, qz = sems
    zh, x, zl, y, core = place()
    t = zl * 8 + y * 2 + core
    xp, xm = (x + 1) % 4, (x + 3) % 4
    right, left = {"plane": zh * 4 + xp, "tile": t}, {"plane": zh * 4 + xm, "tile": t}
    across = {"plane": (1 - zh) * 4 + x, "tile": t}

    barrier = pltpu.get_barrier_semaphore()
    for dev in (right, left, across):
        pl.semaphore_signal(barrier, inc=1, device_id=dev, device_id_type=MESH)

    l0 = lax.broadcasted_iota(jnp.int32, (256, 128), 0)
    lane = lax.broadcasted_iota(jnp.int32, (256, 128), 1)
    ec, es = cos_sin((l0 * 16 + lane).astype(F32) * (1.0 / G))
    ar, ai = jnp.full((256, 128), ab_ref[0, KS - 1]), jnp.zeros((256, 128), F32)
    for j in range(KS - 2, -1, -1):
        ar, ai = rotated(ar, ai, ec, es)
        ar = ar + ab_ref[0, j]
    sr[...] = ar
    si[...] = ai
    m = t * 256 + zh * 128 + lax.broadcasted_iota(jnp.int32, (8, 128), 1)
    ec, es = cos_sin(m.astype(F32) * (1.0 / G))
    tr, ti = jnp.full((8, 128), ab_ref[1, KS - 1]), jnp.zeros((8, 128), F32)
    for j in range(KS - 2, -1, -1):
        tr, ti = rotated(tr, ti, ec, es)
        tr = tr + ab_ref[1, j]
    tr, ti = tr[0:1] * (1.0 / 512.0), ti[0:1] * (1.0 / 512.0)
    ym = jnp.where(m >= G // 2, m - G, m).astype(F32)[0:1] * (0.5 / G)
    ysq = ym * ym
    ws = [w_ref[q, 0:1, :] for q in range(2)]
    row = lax.broadcasted_iota(jnp.int32, (64, 128), 0)

    pl.semaphore_wait(barrier, 3)

    def copy(src, dst, send, recv, device):
        return pltpu.make_async_remote_copy(
            src_ref=src, dst_ref=dst, send_sem=send, recv_sem=recv, device_id=device, device_id_type=MESH
        )

    def step_one(i):
        xo = (x + 2) % 4
        return (
            copy(pb.at[i, 0, xo], r1.at[i, 0], s1.at[i, 0], q1.at[i, 0], right),
            copy(pb.at[i, 1, xo], r1.at[i, 1], s1.at[i, 1], q1.at[i, 1], left),
        )

    def direct(i):
        return (
            copy(pb.at[i, 0, xm], rd.at[i, 0], sd.at[i, 0], qd.at[i, 0], left),
            copy(pb.at[i, 1, xp], rd.at[i, 1], sd.at[i, 1], qd.at[i, 1], right),
        )

    def forward(i):
        return (
            copy(fw.at[i, 0], rc.at[i, 0], sf.at[i, 0], qf.at[i, 0], right),
            copy(fw.at[i, 1], rc.at[i, 1], sf.at[i, 1], qf.at[i, 1], left),
        )

    def over(i):
        return copy(zb.at[i], zr.at[i], sz.at[i], qz.at[i], across)

    def compute(i):
        for q in range(4):
            rows = slice(q * 64, q * 64 + 64)
            l = (row + q * 64) * 16 + i
            xl = jnp.where(l >= G // 2, l - G, l).astype(F32) * (0.5 / G)
            rho = xl * xl + ysq
            n = -rho / (1.0 + jnp.sqrt(1.0 - rho))
            zre = zim = None
            for v in range(2):
                hp = hp_ref[v, i]
                pc = lax.dot_general(dm_ref[rows, :], hp, NT, preferred_element_type=F32)
                ps = lax.dot_general(dm_ref[256 + q * 64 : 320 + q * 64, :], hp, NT, preferred_element_type=F32)
                dre = pc[:, :128] - ps[:, 128:]
                dim = ps[:, :128] + pc[:, 128:]
                c, s = cos_sin(ws[v] * n)
                a, b = rotated(dre, dim, c, s)
                zre, zim = (a, b) if zre is None else (zre + a, zim + b)
            a, b = rotated(zre, zim, tr, ti)
            lanes = lax.broadcasted_iota(jnp.int32, (64, 128), 1)
            cs = jnp.sum(jnp.where(lanes == i, sr[rows], 0.0), axis=1, keepdims=True)
            ss = jnp.sum(jnp.where(lanes == i, si[rows], 0.0), axis=1, keepdims=True)
            part = cs * a - ss * b
            for k in range(2):
                pb[i, q // 2, (q % 2) * 2 + k] = part[k * 32 : k * 32 + 32]

    def put(i, half, value):
        out_ref[pl.ds(half * 512 + i, 32, stride=16), :] = value

    lag1, lag2, lag3 = 4, 8, 12

    def turn(i, _):
        @pl.when(i < 16)
        def _():
            compute(i)
            for c in step_one(i) + direct(i):
                c.start()

        @pl.when(jnp.logical_and(i >= lag1, i < 16 + lag1))
        def _():
            j = i - lag1
            for c in step_one(j):
                c.wait_recv()
            fw[j, 0] = r1[j, 0] + pb[j, 0, xp]
            fw[j, 1] = r1[j, 1] + pb[j, 1, xm]
            for c in forward(j):
                c.start()

        @pl.when(jnp.logical_and(i >= lag2, i < 16 + lag2))
        def _():
            j = i - lag2
            for c in forward(j) + direct(j):
                c.wait_recv()
            put(j, zh, pb[j, zh, x] + rc[j, zh] + rd[j, zh])
            zb[j] = pb[j, 1 - zh, x] + rc[j, 1 - zh] + rd[j, 1 - zh]
            over(j).start()

        @pl.when(i >= lag3)
        def _():
            j = i - lag3
            over(j).wait_recv()
            put(j, 1 - zh, zr[j])

        return 0

    lax.fori_loop(0, 16 + lag3, turn, 0)

    def drain(i, _):
        for c in step_one(i) + direct(i) + forward(i) + (over(i),):
            c.wait_send()
        return 0

    lax.fori_loop(0, 16, drain, 0)


def image_call(ab, hp, w, dm):
    dma = pltpu.SemaphoreType.DMA
    vmem = pl.BlockSpec(memory_space=pltpu.VMEM)
    buf = pltpu.VMEM((16, 2, 32, 128), F32)
    half = pltpu.VMEM((16, 32, 128), F32)
    return pl.pallas_call(
        image_kernel,
        out_shape=jax.ShapeDtypeStruct((1024, 128), F32),
        in_specs=[pl.BlockSpec(memory_space=pltpu.SMEM), vmem, vmem, vmem],
        out_specs=vmem,
        scratch_shapes=[pltpu.VMEM((256, 128), F32)] * 2
        + [pltpu.VMEM((16, 2, 4, 32, 128), F32), buf, buf, buf, buf, half, half]
        + [dma((16, 2))] * 6
        + [dma((16,))] * 2,
        compiler_params=pltpu.CompilerParams(collective_id=1, has_side_effects=True, vmem_limit_bytes=32 << 20),
        name="imagesum",
    )(ab, hp, w, dm)


def constants():
    k = np.arange(256)
    a = 2 * np.pi * (np.outer(k, k) % 256) / 256
    dm = np.concatenate([np.cos(a), np.sin(a)], axis=0)
    b = 2 * np.pi * np.outer(np.arange(16), k) / G
    return dm.astype(jnp.bfloat16), np.stack([np.cos(b), np.sin(b)]).astype(np.float32)


def local(visibility, target, offset, taps, w_plane):
    dm, tw = constants()
    count = visibility.shape[1]
    s = sort_call(visibility, target.reshape(1, count), offset.reshape(1, count))
    w = jnp.broadcast_to(w_plane.reshape(1, 1), (8, 128))
    ga, wo = exchange_call(s.reshape(2, 4, 16, 128), w)
    mb = lax.axis_index("tile") * 256 + (lax.axis_index("plane") // 4) * 128
    hp = grid_call(mb.astype(F32).reshape(1), ga.reshape(32 * 96, 128), jnp.asarray(tw))
    ab = jnp.stack([taps, lax.reduce_precision(taps, 8, 7)])
    halves = image_call(ab, hp, wo, jnp.asarray(dm))
    return jnp.concatenate([halves[:512], halves[512:]], axis=1)


def solution(mesh):
    planes, tiles = ("plane",), ("tile",)
    both = planes + tiles
    return jax.shard_map(
        local,
        mesh=mesh,
        in_specs=(P(None, both), P(both, None), P(both), P(), P("plane")),
        out_specs=P("plane", "tile"),
        check_vma=False,
    )
```

```python
import math

import jax
import jax.numpy as jnp
import numpy as np
from jax import lax
from jax.experimental import pallas as pl
from jax.experimental.pallas import tpu as pltpu
from jax.sharding import PartitionSpec as P


G = 4096
KS = 8
MESH = pl.DeviceIdType.MESH
F32 = jnp.float32
BF16 = jnp.bfloat16
NT = (((1,), (1,)), ((), ()))

SIN = (3.1415927410125732, -5.167710304260254, 2.550077438354492, -0.598291277885437, 0.07765766233205795)
COS = (0.9999999403953552, -4.934792995452881, 4.058411121368408, -1.331876516342163, 0.21968960762023926)


def poly(coefs, g):
    out = g * coefs[-1] + coefs[-2]
    for c in coefs[-3::-1]:
        out = out * g + c
    return out


def cos_sin(cycles):
    f = cycles - jnp.floor(cycles + 0.5)
    g = f * f
    s = f * poly(SIN, g)
    c = poly(COS, g)
    s2 = s + s
    return 1.0 - s2 * s, s2 * c


def rotated(re, im, c, s):
    return re * c - im * s, re * s + im * c


def dft(re, im):
    n = len(re)
    if n == 1:
        return re, im
    er, ei = dft(re[0::2], im[0::2])
    dr, di = dft(re[1::2], im[1::2])
    h = n // 2
    out_r, out_i = [None] * n, [None] * n
    for k in range(h):
        if k == 0:
            tr, ti = dr[k], di[k]
        elif 4 * k == n:
            tr, ti = -di[k], dr[k]
        elif 8 * k == n:
            q = math.sqrt(0.5)
            tr, ti = (dr[k] - di[k]) * q, (dr[k] + di[k]) * q
        elif 8 * k == 3 * n:
            q = math.sqrt(0.5)
            tr, ti = (dr[k] + di[k]) * -q, (dr[k] - di[k]) * q
        else:
            c, s = math.cos(2 * math.pi * k / n), math.sin(2 * math.pi * k / n)
            tr, ti = dr[k] * c - di[k] * s, dr[k] * s + di[k] * c
        out_r[k], out_i[k] = er[k] + tr, ei[k] + ti
        out_r[k + h], out_i[k + h] = er[k] - tr, ei[k] - ti
    return out_r, out_i


def sort(vis_ref, tgt_ref, off_ref, out_ref):
    count = tgt_ref.shape[1]
    blk = 256
    ii = lax.broadcasted_iota(jnp.int32, (blk, blk), 0)
    jj = lax.broadcasted_iota(jnp.int32, (blk, blk), 1)
    tri = jnp.where(ii < jj, 1.0, 0.0).astype(BF16)
    rows = lax.broadcasted_iota(jnp.int32, (128, blk), 0)
    ranks = lax.broadcasted_iota(jnp.int32, (32, blk), 0).astype(F32)
    carry = jnp.zeros((128, 1), F32)
    acc = jnp.zeros((128, 128), F32)
    for b in range(count // blk):
        sl = slice(b * blk, (b + 1) * blk)
        one = jnp.where(rows == tgt_ref[:, sl], 1.0, 0.0)
        oneb = one.astype(BF16)
        before = jnp.dot(oneb, tri, preferred_element_type=F32)
        rank = jnp.sum(one * (before + carry), axis=0, keepdims=True)
        carry = carry + jnp.sum(one, axis=1, keepdims=True)
        hit = ranks == rank
        off = off_ref[:, sl]
        parts = [((off >> 12) << 12).astype(F32), (((off >> 4) & 255) << 4).astype(F32), (off & 15).astype(F32)]
        left = [vis_ref[0:1, sl], vis_ref[1:2, sl]]
        for k in range(3):
            cols = []
            for v in range(2):
                top = left[v].astype(BF16).astype(F32)
                left[v] = left[v] - top
                cols.append(jnp.where(hit, top, 0.0))
            cols.append(jnp.where(hit, parts[k], 0.0))
            cols.append(jnp.zeros((32, blk), F32))
            table = jnp.concatenate(cols, axis=0).astype(BF16)
            acc = acc + lax.dot_general(oneb, table, NT, preferred_element_type=F32)
    for q in range(8):
        out_ref[q // 4, q % 4] = acc[q * 16 : q * 16 + 16]


def place():
    p = lax.axis_index("plane")
    t = lax.axis_index("tile")
    return p // 4, p % 4, t // 8, (t // 2) % 4, t % 2


def kernel(w_ref, ab_ref, vis_ref, tgt_ref, off_ref, tw_ref, dm_ref, out_ref, *scratch):
    sb, wb, wo, ra, ga, hs, hp, xs, ts, rs, sr, si, pb, r1, fw, rc, rd, zb, zr = scratch[:19]
    sa, qa, sy, qy, sv, qv, sc, qc, sw, qw, s1, q1, sf, qf, sd, qd, sz, qz = scratch[19:]
    zh, x, zl, y, core = place()
    z = zh * 2 + zl
    p, t = zh * 4 + x, zl * 8 + y * 2 + core
    xp, xm = (x + 1) % 4, (x + 3) % 4

    def at_x(d):
        return {"plane": zh * 4 + (x + d) % 4, "tile": t}

    def at_y(d):
        return {"plane": p, "tile": zl * 8 + ((y + d) % 4) * 2 + core}

    def at_z(d):
        zz = (z + d) % 4
        return {"plane": (zz // 2) * 4 + x, "tile": (zz % 2) * 8 + y * 2 + core}

    partner = {"plane": p, "tile": zl * 8 + y * 2 + (1 - core)}
    right, left, across = at_x(1), at_x(3), at_z(2)

    barrier = pltpu.get_barrier_semaphore()
    for d in (1, 2, 3):
        for at in (at_x, at_y, at_z):
            pl.semaphore_signal(barrier, inc=1, device_id=at(d), device_id_type=MESH)
    pl.semaphore_signal(barrier, inc=1, device_id=partner, device_id_type=MESH)

    def copy(src, dst, send, recv, device):
        return pltpu.make_async_remote_copy(
            src_ref=src, dst_ref=dst, send_sem=send, recv_sem=recv, device_id=device, device_id_type=MESH
        )

    sort(vis_ref, tgt_ref, off_ref, sb)
    wb[...] = jnp.full((8, 128), w_ref[0])
    wo[zh] = wb[...]
    pl.semaphore_wait(barrier, 10)
    first = [copy(sb.at[:, (x + d) % 4], ra.at[x], sa.at[d - 1], qa.at[d - 1], at_x(d)) for d in (1, 2, 3)]
    for c in first:
        c.start()
    ra[x] = sb[:, x]

    l0 = lax.broadcasted_iota(jnp.int32, (256, 128), 0)
    lane = lax.broadcasted_iota(jnp.int32, (256, 128), 1)
    ec, es = cos_sin((l0 * 16 + lane).astype(F32) * (1.0 / G))
    ar, ai = jnp.full((256, 128), ab_ref[0, KS - 1]), jnp.zeros((256, 128), F32)
    for j in range(KS - 2, -1, -1):
        ar, ai = rotated(ar, ai, ec, es)
        ar = ar + ab_ref[0, j]
    sr[...] = ar
    si[...] = ai

    for c in first:
        c.wait()

    def rows_of(zrow, cr):
        return ga.at[pl.ds(pl.multiple_of((zrow * 2 + cr) * 384, 384), 384)]

    got = [ra[s].reshape(32, 128) for s in range(4)]
    group = lax.broadcasted_iota(jnp.int32, (32, 128), 1) // 32
    base = pl.multiple_of(((z * 2 + core) * 4 + y) * 96, 96)
    for k in range(3):
        row = jnp.zeros((32, 128), F32)
        for s in range(4):
            shift = (32 * (s - k)) % 128
            moved = pltpu.roll(got[s], shift, 1) if shift else got[s]
            row = jnp.where(group == s, moved, row)
        ga[pl.ds(base + k * 16, 16)] = row[:16]
        ga[pl.ds(base + 48 + k * 16, 16)] = row[16:]
    mine = ga.at[pl.ds(base, 96)]
    ring = [copy(mine, mine, sy.at[d - 1], qy.at[d - 1], at_y(d)) for d in (1, 3, 2)]
    for c in ring:
        c.start()
    wcopy = copy(wb, wo.at[zh], sw, qw, across)
    wcopy.start()

    def clear(i, _):
        hs[i // 16, i % 16] = jnp.zeros((256, 256), F32)
        return 0

    lax.fori_loop(0, 32, clear, 0)
    for c in ring:
        c.wait()

    def zrow_of(g):
        return (z + jnp.where(g == 0, 0, jnp.where(g == 1, 3, g - 1))) % 4

    own = rows_of(z, core)
    rings = [copy(own, own, sv.at[g], qv.at[g], at_z(d)) for g, d in ((0, 1), (1, 3), (2, 2))]

    def arrival(g):
        part = rows_of(zrow_of(g), core)
        return copy(part, part, sv.at[g - 1], qv.at[g - 1], across)

    def swap(g):
        part = rows_of(zrow_of(g), core)
        return copy(part, part, sc.at[g], qc.at[g], partner)

    def swapped(g):
        part = rows_of(zrow_of(g), 1 - core)
        return copy(part, part, sc.at[g], qc.at[g], partner)

    swap(0).start()
    for c in rings:
        c.start()

    mb = (t * 256 + zh * 128).astype(F32)
    sub = lax.broadcasted_iota(jnp.int32, (8, 128), 0).astype(F32)

    def dense(start, u):
        re = ga[pl.ds(start, 8, stride=96), :]
        im = ga[pl.ds(start + 16, 8, stride=96), :]
        off = ga[pl.ds(start + 32, 8, stride=96), :]
        row = jnp.floor(off * (1.0 / G))
        col = off - row * G
        cb, sb_ = cos_sin(col * mb * (1.0 / G))
        c1, s1_ = cos_sin(col * (1.0 / G))
        c8, s8 = cos_sin(col * (8.0 / G))
        re, im = rotated(re, im, cb, sb_)
        for s in range(8):
            nr, ni = rotated(re, im, c8, s8)
            xs[u, 0, s * 8 : s * 8 + 8] = re
            xs[u, 1, s * 8 : s * 8 + 8] = im
            xs[u, 2, s * 8 : s * 8 + 8] = nr
            xs[u, 3, s * 8 : s * 8 + 8] = ni
            if s < 7:
                re, im = rotated(re, im, c1, s1_)
        ts[u] = c8 + c8
        rs[u] = row

    def product(u):
        tabs, hots = [], []
        for dev in range(8):
            turn = jnp.broadcast_to(ts[u, dev : dev + 1, :], (8, 128))
            rows = []
            for v in range(2):
                a = xs[u, v, pl.ds(dev, 8, stride=8), :]
                b = xs[u, 2 + v, pl.ds(dev, 8, stride=8), :]
                for k in range(16):
                    rows.append(a)
                    a, b = b, turn * b - a
            tabs.append(jnp.concatenate(rows, axis=0))
            r = jnp.broadcast_to(rs[u, dev : dev + 1, :], (8, 128)) - sub
            r = jnp.concatenate([r, r - 8.0], axis=0).astype(BF16)
            one, zero = jnp.ones((), BF16), jnp.zeros((), BF16)
            hots.append(
                jnp.concatenate([jnp.where(r == jnp.asarray(16.0 * j, BF16), one, zero) for j in range(16)], axis=0)
            )
        tab, hot = jnp.concatenate(tabs, axis=1), jnp.concatenate(hots, axis=1)
        return lax.dot_general(tab, hot, NT, preferred_element_type=F32)

    def segment(n, _):
        g, half = n // 2, n % 2

        @pl.when(jnp.logical_and(half == 1, g < 3))
        def _():
            arrival(g + 1).wait_recv()
            swap(g + 1).start()

        @pl.when(half == 0)
        def _():
            swapped(g).wait_recv()

        start = zrow_of(g) * 768 + half * 48
        for u in range(4):
            dense(start + u, u)

        def quad(it, _):
            for u in range(4):
                hs[half, it * 4 + u] += product(u)
            following = start + jnp.minimum(it + 1, 3) * 4
            for u in range(4):
                dense(following + u, u)
            return 0

        lax.fori_loop(0, 4, quad, 0)
        return 0

    lax.fori_loop(0, 8, segment, 0)

    def strip(i, _):
        v = i // 8
        m = pl.multiple_of(i % 8 * 16, 16)
        for h in range(2):
            lanes = slice(h * 128, h * 128 + 128)
            re = [hs[v, b, pl.ds(m, 16), lanes] for b in range(16)]
            im = [hs[v, b, pl.ds(m + 128, 16), lanes] for b in range(16)]
            re, im = dft(re, im)
            for q in range(16):
                a, b = re[q], im[q]
                if q:
                    a, b = rotated(a, b, tw_ref[0, q : q + 1, lanes], tw_ref[1, q : q + 1, lanes])
                hp[v, q, pl.ds(m, 16), lanes] = a.astype(BF16)
                hp[v, q, pl.ds(m + 128, 16), lanes] = b.astype(BF16)
        return 0

    lax.fori_loop(0, 16, strip, 0)
    wcopy.wait()

    m = t * 256 + zh * 128 + lax.broadcasted_iota(jnp.int32, (8, 128), 1)
    ec, es = cos_sin(m.astype(F32) * (1.0 / G))
    tr, ti = jnp.full((8, 128), ab_ref[1, KS - 1]), jnp.zeros((8, 128), F32)
    for j in range(KS - 2, -1, -1):
        tr, ti = rotated(tr, ti, ec, es)
        tr = tr + ab_ref[1, j]
    tr, ti = tr[0:1] * (1.0 / 512.0), ti[0:1] * (1.0 / 512.0)
    ym = jnp.where(m >= G // 2, m - G, m).astype(F32)[0:1] * (0.5 / G)
    ysq = ym * ym
    ws = [wo[q, 0:1, :] for q in range(2)]
    row64 = lax.broadcasted_iota(jnp.int32, (64, 128), 0)
    lane64 = lax.broadcasted_iota(jnp.int32, (64, 128), 1)

    def step_one(i):
        xo = (x + 2) % 4
        return (
            copy(pb.at[i, 0, xo], r1.at[i, 0], s1.at[i, 0], q1.at[i, 0], right),
            copy(pb.at[i, 1, xo], r1.at[i, 1], s1.at[i, 1], q1.at[i, 1], left),
        )

    def direct(i):
        return (
            copy(pb.at[i, 0, xm], rd.at[i, 0], sd.at[i, 0], qd.at[i, 0], left),
            copy(pb.at[i, 1, xp], rd.at[i, 1], sd.at[i, 1], qd.at[i, 1], right),
        )

    def forward(i):
        return (
            copy(fw.at[i, 0], rc.at[i, 0], sf.at[i, 0], qf.at[i, 0], right),
            copy(fw.at[i, 1], rc.at[i, 1], sf.at[i, 1], qf.at[i, 1], left),
        )

    def over(i):
        return copy(zb.at[i], zr.at[i], sz.at[i], qz.at[i], across)

    def compute(i):
        for q in range(4):
            rows = slice(q * 64, q * 64 + 64)
            l = (row64 + q * 64) * 16 + i
            xl = jnp.where(l >= G // 2, l - G, l).astype(F32) * (0.5 / G)
            rho = xl * xl + ysq
            n = -rho / (1.0 + jnp.sqrt(1.0 - rho))
            zre = zim = None
            for v in range(2):
                h = hp[v, i]
                pc = lax.dot_general(dm_ref[rows, :], h, NT, preferred_element_type=F32)
                ps = lax.dot_general(dm_ref[256 + q * 64 : 320 + q * 64, :], h, NT, preferred_element_type=F32)
                dre = pc[:, :128] - ps[:, 128:]
                dim = ps[:, :128] + pc[:, 128:]
                c, s = cos_sin(ws[v] * n)
                a, b = rotated(dre, dim, c, s)
                zre, zim = (a, b) if zre is None else (zre + a, zim + b)
            a, b = rotated(zre, zim, tr, ti)
            cs = jnp.sum(jnp.where(lane64 == i, sr[rows], 0.0), axis=1, keepdims=True)
            ss = jnp.sum(jnp.where(lane64 == i, si[rows], 0.0), axis=1, keepdims=True)
            part = cs * a - ss * b
            for k in range(2):
                pb[i, q // 2, (q % 2) * 2 + k] = part[k * 32 : k * 32 + 32]

    def put(i, half, value):
        out_ref[pl.ds(half * 512 + i, 32, stride=16), :] = value

    lag1, lag2, lag3 = 4, 8, 12

    def turn(i, _):
        @pl.when(i < 16)
        def _():
            compute(i)
            for c in step_one(i) + direct(i):
                c.start()

        @pl.when(jnp.logical_and(i >= lag1, i < 16 + lag1))
        def _():
            j = i - lag1
            for c in step_one(j):
                c.wait_recv()
            fw[j, 0] = r1[j, 0] + pb[j, 0, xp]
            fw[j, 1] = r1[j, 1] + pb[j, 1, xm]
            for c in forward(j):
                c.start()

        @pl.when(jnp.logical_and(i >= lag2, i < 16 + lag2))
        def _():
            j = i - lag2
            for c in forward(j) + direct(j):
                c.wait_recv()
            put(j, zh, pb[j, zh, x] + rc[j, zh] + rd[j, zh])
            zb[j] = pb[j, 1 - zh, x] + rc[j, 1 - zh] + rd[j, 1 - zh]
            over(j).start()

        @pl.when(i >= lag3)
        def _():
            j = i - lag3
            over(j).wait_recv()
            put(j, 1 - zh, zr[j])

        return 0

    lax.fori_loop(0, 16 + lag3, turn, 0)

    def drain(i, _):
        for c in step_one(i) + direct(i) + forward(i) + (over(i),):
            c.wait_send()
        return 0

    lax.fori_loop(0, 16, drain, 0)
    for c in rings:
        c.wait_send()
    for g in range(4):
        swap(g).wait_send()

def constants():
    k = np.arange(256)
    a = 2 * np.pi * (np.outer(k, k) % 256) / 256
    dm = np.concatenate([np.cos(a), np.sin(a)], axis=0)
    b = 2 * np.pi * np.outer(np.arange(16), k) / G
    return dm.astype(jnp.bfloat16), np.stack([np.cos(b), np.sin(b)]).astype(np.float32)

def local(visibility, target, offset, taps, w_plane):
    dm, tw = constants()
    count = visibility.shape[1]
    ab = jnp.stack([taps, lax.reduce_precision(taps, 8, 7)])
    dma = pltpu.SemaphoreType.DMA
    vmem = pl.BlockSpec(memory_space=pltpu.VMEM)
    smem = pl.BlockSpec(memory_space=pltpu.SMEM)
    buf = pltpu.VMEM((16, 2, 32, 128), F32)
    part = pltpu.VMEM((16, 32, 128), F32)
    halves = pl.pallas_call(
        kernel,
        out_shape=jax.ShapeDtypeStruct((1024, 128), F32),
        in_specs=[smem, smem] + [vmem] * 5,
        out_specs=vmem,
        scratch_shapes=[
            pltpu.VMEM((2, 4, 16, 128), F32),
            pltpu.VMEM((8, 128), F32),
            pltpu.VMEM((2, 8, 128), F32),
            pltpu.VMEM((4, 2, 16, 128), F32),
            pltpu.VMEM((3072, 128), F32),
            pltpu.VMEM((2, 16, 256, 256), F32),
            pltpu.VMEM((2, 16, 256, 256), BF16),
            pltpu.VMEM((4, 4, 64, 128), F32),
            pltpu.VMEM((4, 8, 128), F32),
            pltpu.VMEM((4, 8, 128), F32),
            pltpu.VMEM((256, 128), F32),
            pltpu.VMEM((256, 128), F32),
            pltpu.VMEM((16, 2, 4, 32, 128), F32),
            buf,
            buf,
            buf,
            buf,
            part,
            part,
        ]
        + [dma((3,))] * 6
        + [dma((4,))] * 2
        + [dma] * 2
        + [dma((16, 2))] * 6
        + [dma((16,))] * 2,
        compiler_params=pltpu.CompilerParams(collective_id=0, has_side_effects=True, vmem_limit_bytes=56 << 20),
        name="dirtyimage",
    )(w_plane, ab, visibility, target.reshape(1, count), offset.reshape(1, count), jnp.asarray(tw), jnp.asarray(dm))
    return jnp.concatenate([halves[:512], halves[512:]], axis=1)


def solution(mesh):
    both = ("plane", "tile")
    return jax.shard_map(
        local,
        mesh=mesh,
        in_specs=(P(None, both), P(both, None), P(both), P(), P("plane")),
        out_specs=P("plane", "tile"),
        check_vma=False,
    )
```

```python
import math

import jax
import jax.numpy as jnp
from jax import lax
from jax.experimental import pallas as pl
from jax.experimental.pallas import tpu as pltpu
from jax.sharding import PartitionSpec as P


G = 4096
KS = 8
MESH = pl.DeviceIdType.MESH
F32 = jnp.float32
BF16 = jnp.bfloat16
NT = (((1,), (1,)), ((), ()))

SIN = (3.1415927410125732, -5.167710304260254, 2.550077438354492, -0.598291277885437, 0.07765766233205795)
COS = (0.9999999403953552, -4.934792995452881, 4.058411121368408, -1.331876516342163, 0.21968960762023926)


def poly(coefs, g):
    out = g * coefs[-1] + coefs[-2]
    for c in coefs[-3::-1]:
        out = out * g + c
    return out


def cos_sin(cycles):
    f = cycles - jnp.floor(cycles + 0.5)
    g = f * f
    s = f * poly(SIN, g)
    c = poly(COS, g)
    s2 = s + s
    return 1.0 - s2 * s, s2 * c


def rotated(re, im, c, s):
    return re * c - im * s, re * s + im * c


def dft(re, im):
    n = len(re)
    if n == 1:
        return re, im
    er, ei = dft(re[0::2], im[0::2])
    dr, di = dft(re[1::2], im[1::2])
    h = n // 2
    out_r, out_i = [None] * n, [None] * n
    for k in range(h):
        if k == 0:
            tr, ti = dr[k], di[k]
        elif 4 * k == n:
            tr, ti = -di[k], dr[k]
        elif 8 * k == n:
            q = math.sqrt(0.5)
            tr, ti = (dr[k] - di[k]) * q, (dr[k] + di[k]) * q
        elif 8 * k == 3 * n:
            q = math.sqrt(0.5)
            tr, ti = (dr[k] + di[k]) * -q, (dr[k] - di[k]) * q
        else:
            c, s = math.cos(2 * math.pi * k / n), math.sin(2 * math.pi * k / n)
            tr, ti = dr[k] * c - di[k] * s, dr[k] * s + di[k] * c
        out_r[k], out_i[k] = er[k] + tr, ei[k] + ti
        out_r[k + h], out_i[k + h] = er[k] - tr, ei[k] - ti
    return out_r, out_i


def sort(vis_ref, tgt_ref, off_ref, out_ref):
    count = tgt_ref.shape[1]
    blk = 256
    ii = lax.broadcasted_iota(jnp.int32, (blk, blk), 0)
    jj = lax.broadcasted_iota(jnp.int32, (blk, blk), 1)
    tri = jnp.where(ii < jj, 1.0, 0.0).astype(BF16)
    rows = lax.broadcasted_iota(jnp.int32, (128, blk), 0)
    ranks = lax.broadcasted_iota(jnp.int32, (32, blk), 0).astype(F32)
    carry = jnp.zeros((128, 1), F32)
    acc = jnp.zeros((128, 128), F32)
    for b in range(count // blk):
        sl = slice(b * blk, (b + 1) * blk)
        one = jnp.where(rows == tgt_ref[:, sl], 1.0, 0.0)
        oneb = one.astype(BF16)
        before = jnp.dot(oneb, tri, preferred_element_type=F32)
        rank = jnp.sum(one * (before + carry), axis=0, keepdims=True)
        carry = carry + jnp.sum(one, axis=1, keepdims=True)
        hit = ranks == rank
        off = off_ref[:, sl]
        parts = [((off >> 12) << 12).astype(F32), (((off >> 4) & 255) << 4).astype(F32), (off & 15).astype(F32)]
        left = [vis_ref[0:1, sl], vis_ref[1:2, sl]]
        for k in range(3):
            cols = []
            for v in range(2):
                top = left[v].astype(BF16).astype(F32)
                left[v] = left[v] - top
                cols.append(jnp.where(hit, top, 0.0))
            cols.append(jnp.where(hit, parts[k], 0.0))
            cols.append(jnp.zeros((32, blk), F32))
            table = jnp.concatenate(cols, axis=0).astype(BF16)
            acc = acc + lax.dot_general(oneb, table, NT, preferred_element_type=F32)
    for q in range(8):
        out_ref[q // 4, q % 4] = acc[q * 16 : q * 16 + 16]


def place():
    p = lax.axis_index("plane")
    t = lax.axis_index("tile")
    return p // 4, p % 4, t // 8, (t // 2) % 4, t % 2


def kernel(w_ref, taps_ref, vis_ref, tgt_ref, off_ref, out_ref, *scratch):
    sb, wb, wo, ra, ga, hs, hp, eq, dm, tw, xs, ts, rs, sr, si, pb, r1, fw, rc, rd, zb, zr = scratch[:22]
    sa, qa, sn, qn, sv, qv, sc, qc, sw, qw, s1, q1, sf, qf, sd, qd, sz, qz = scratch[22:]
    zh, x, zl, y, core = place()
    z = zh * 2 + zl
    p, t = zh * 4 + x, zl * 8 + y * 2 + core
    xp, xm = (x + 1) % 4, (x + 3) % 4

    def at_x(d):
        return {"plane": zh * 4 + (x + d) % 4, "tile": t}

    def at_y(d):
        return {"plane": p, "tile": zl * 8 + ((y + d) % 4) * 2 + core}

    def at_z(d):
        zz = (z + d) % 4
        return {"plane": (zz // 2) * 4 + x, "tile": (zz % 2) * 8 + y * 2 + core}

    partner = {"plane": p, "tile": zl * 8 + y * 2 + (1 - core)}
    right, left, across = at_x(1), at_x(3), at_z(2)

    barrier = pltpu.get_barrier_semaphore()
    for d in (1, 2, 3):
        for at in (at_x, at_y, at_z):
            pl.semaphore_signal(barrier, inc=1, device_id=at(d), device_id_type=MESH)
    pl.semaphore_signal(barrier, inc=1, device_id=partner, device_id_type=MESH)

    def copy(src, dst, send, recv, device):
        return pltpu.make_async_remote_copy(
            src_ref=src, dst_ref=dst, send_sem=send, recv_sem=recv, device_id=device, device_id_type=MESH
        )

    sort(vis_ref, tgt_ref, off_ref, sb)
    wb[...] = jnp.full((8, 128), w_ref[0])
    wo[zh] = wb[...]
    pl.semaphore_wait(barrier, 10)
    first = [copy(sb.at[:, (x + d) % 4], ra.at[x], sa.at[d - 1], qa.at[d - 1], at_x(d)) for d in (1, 3, 2)]
    for c in first:
        c.start()
    wcopy = copy(wb, wo.at[zh], sw, qw, across)
    wcopy.start()
    ra[x] = sb[:, x]

    l0 = lax.broadcasted_iota(jnp.int32, (256, 128), 0)
    lane = lax.broadcasted_iota(jnp.int32, (256, 128), 1)
    ec, es = cos_sin((l0 * 16 + lane).astype(F32) * (1.0 / G))
    ar, ai = jnp.full((256, 128), taps_ref[KS - 1]), jnp.zeros((256, 128), F32)
    for j in range(KS - 2, -1, -1):
        ar, ai = rotated(ar, ai, ec, es)
        ar = ar + taps_ref[j]
    sr[...] = ar
    si[...] = ai
    m = t * 256 + zh * 128 + lax.broadcasted_iota(jnp.int32, (8, 128), 1)
    ec, es = cos_sin(m.astype(F32) * (1.0 / G))
    taps_low = [jnp.full((8, 128), taps_ref[j]).astype(BF16).astype(F32) for j in range(KS)]
    tr, ti = taps_low[KS - 1], jnp.zeros((8, 128), F32)
    for j in range(KS - 2, -1, -1):
        tr, ti = rotated(tr, ti, ec, es)
        tr = tr + taps_low[j]
    tr, ti = tr[0:1] * (1.0 / 512.0), ti[0:1] * (1.0 / 512.0)
    ym = jnp.where(m >= G // 2, m - G, m).astype(F32)[0:1] * (0.5 / G)
    ysq = ym * ym
    row64 = lax.broadcasted_iota(jnp.int32, (64, 128), 0)
    lane64 = lax.broadcasted_iota(jnp.int32, (64, 128), 1)

    def screen(n, _):
        v = jnp.where(n < 16, zh, 1 - zh)
        i = n % 16
        w = wo[v, 0:1, :]
        for q in range(4):
            rows = slice(q * 64, q * 64 + 64)
            l = (row64 + q * 64) * 16 + i
            xl = jnp.where(l >= G // 2, l - G, l).astype(F32) * (0.5 / G)
            rho = xl * xl + ysq
            n_minus = -rho / (1.0 + jnp.sqrt(1.0 - rho))
            c, s = cos_sin(w * n_minus)
            c, s = rotated(c, s, tr, ti)
            cs = jnp.sum(jnp.where(lane64 == i, sr[rows], 0.0), axis=1, keepdims=True)
            ss = jnp.sum(jnp.where(lane64 == i, si[rows], 0.0), axis=1, keepdims=True)
            c, s = rotated(c, s, cs, ss)
            eq[v, i, 0, rows] = c
            eq[v, i, 1, rows] = s
        return 0

    lax.fori_loop(0, 12, screen, 0)
    for c in first:
        c.wait()

    outer, inner = (z, y), (y, z)
    around = ((at_y, at_z), (at_z, at_y))

    def rows_of(h, g, cr):
        step = jnp.where(g == 0, 0, jnp.where(g == 1, 3, g - 1))
        o = (outer[h] + step) % 4
        return ga.at[pl.ds(pl.multiple_of(h * 1536 + (o * 2 + cr) * 192, 192), 192)]

    got = [ra[s].reshape(32, 128) for s in range(4)]
    group = lax.broadcasted_iota(jnp.int32, (32, 128), 1) // 32
    base = [pl.multiple_of(h * 1536 + ((outer[h] * 2 + core) * 4 + inner[h]) * 48, 48) for h in range(2)]
    for k in range(3):
        row = jnp.zeros((32, 128), F32)
        for s in range(4):
            shift = (32 * (s - k)) % 128
            moved = pltpu.roll(got[s], shift, 1) if shift else got[s]
            row = jnp.where(group == s, moved, row)
        for h in range(2):
            ga[pl.ds(base[h] + k * 16, 16)] = row[h * 16 : h * 16 + 16]
    near = []
    for d in (1, 3, 2):
        for h in range(2):
            mine = ga.at[pl.ds(base[h], 48)]
            near.append(copy(mine, mine, sn.at[h, d - 1], qn.at[h, d - 1], around[h][0](d)))
    for c in near:
        c.start()
    wcopy.wait()
    lax.fori_loop(12, 24, screen, 0)
    for q in range(8):
        a = lax.broadcasted_iota(jnp.int32, (32, 256), 0) + q * 32
        b = lax.broadcasted_iota(jnp.int32, (32, 256), 1)
        c, s = cos_sin(((a * b) % 256).astype(F32) * (1.0 / 256.0))
        dm[q * 32 : q * 32 + 32] = c.astype(BF16)
        dm[256 + q * 32 : 288 + q * 32] = s.astype(BF16)
    a = lax.broadcasted_iota(jnp.int32, (16, 256), 0)
    b = lax.broadcasted_iota(jnp.int32, (16, 256), 1)
    c, s = cos_sin((a * b).astype(F32) * (1.0 / G))
    tw[0] = c
    tw[1] = s
    for c in near:
        c.wait()

    far = []
    for g, d in ((1, 1), (2, 3), (3, 2)):
        for h in range(2):
            own = rows_of(h, 0, core)
            far.append(copy(own, own, sv.at[h, g], qv.at[h, g], around[h][1](d)))

    def arrival(h, g):
        part = rows_of(h, g, core)
        return copy(part, part, sv.at[h, g], qv.at[h, g], across)

    def swap(h, g):
        part = rows_of(h, g, core)
        return copy(part, part, sc.at[h, g], qc.at[h, g], partner)

    def swapped(h, g):
        part = rows_of(h, g, 1 - core)
        return copy(part, part, sc.at[h, g], qc.at[h, g], partner)

    for h in range(2):
        swap(h, 0).start()
    for c in far:
        c.start()

    mb = (t * 256 + zh * 128).astype(F32)
    sub = lax.broadcasted_iota(jnp.int32, (8, 128), 0).astype(F32)

    def start_of(h, g):
        step = jnp.where(g == 0, 0, jnp.where(g == 1, 3, g - 1))
        o = (jnp.where(h == 0, outer[0], outer[1]) + step) % 4
        return h * 1536 + o * 384

    def dense(start, u):
        re = ga[pl.ds(start, 8, stride=48), :]
        im = ga[pl.ds(start + 16, 8, stride=48), :]
        off = ga[pl.ds(start + 32, 8, stride=48), :]
        row = jnp.floor(off * (1.0 / G))
        col = off - row * G
        cb, sb_ = cos_sin(col * mb * (1.0 / G))
        c1, s1_ = cos_sin(col * (1.0 / G))
        c8, s8 = cos_sin(col * (8.0 / G))
        re, im = rotated(re, im, cb, sb_)
        for s in range(8):
            nr, ni = rotated(re, im, c8, s8)
            xs[u, 0, s * 8 : s * 8 + 8] = re
            xs[u, 1, s * 8 : s * 8 + 8] = im
            xs[u, 2, s * 8 : s * 8 + 8] = nr
            xs[u, 3, s * 8 : s * 8 + 8] = ni
            if s < 7:
                re, im = rotated(re, im, c1, s1_)
        ts[u] = c8 + c8
        rs[u] = row

    def product(u):
        tabs, hots = [], []
        for dev in range(8):
            turn = jnp.broadcast_to(ts[u, dev : dev + 1, :], (8, 128))
            rows = []
            for v in range(2):
                a = xs[u, v, pl.ds(dev, 8, stride=8), :]
                b = xs[u, 2 + v, pl.ds(dev, 8, stride=8), :]
                for k in range(16):
                    rows.append(a)
                    a, b = b, turn * b - a
            tabs.append(jnp.concatenate(rows, axis=0))
            r = jnp.broadcast_to(rs[u, dev : dev + 1, :], (8, 128)) - sub
            hots.append(jnp.concatenate([jnp.where(r == 8.0 * j, 1.0, 0.0) for j in range(32)], axis=0))
        return tabs, hots

    def total(us):
        tabs, hots = [], []
        for u in us:
            a, b = product(u)
            tabs += a
            hots += b
        tab, hot = jnp.concatenate(tabs, axis=1), jnp.concatenate(hots, axis=1)
        return lax.dot_general(tab, hot, NT, preferred_element_type=F32)

    def early(h, _):
        start = start_of(h, 0)

        def quad(it, _):
            for u in range(4):
                dense(start + it * 4 + u, u)
            for u in range(4):
                hs[h, it * 4 + u] = total([u])
            return 0

        lax.fori_loop(0, 4, quad, 0)
        return 0

    for h in range(2):
        swapped(h, 0).wait_recv()
    lax.fori_loop(0, 2, early, 0)
    for g in (1, 2):
        for h in range(2):
            arrival(h, g).wait_recv()
            swap(h, g).start()
    lax.fori_loop(24, 32, screen, 0)
    for h in range(2):
        arrival(h, 3).wait_recv()
        swap(h, 3).start()
    for g in (1, 2, 3):
        for h in range(2):
            swapped(h, g).wait_recv()

    def late(h, _):
        starts = [start_of(h, g) for g in (1, 2, 3)]
        for u in range(3):
            dense(starts[u], u)

        def one(band, _):
            hs[h, band] += total([0, 1, 2])
            following = jnp.minimum(band + 1, 15)
            for u in range(3):
                dense(starts[u] + following, u)
            return 0

        lax.fori_loop(0, 16, one, 0)
        return 0

    lax.fori_loop(0, 2, late, 0)

    def strip(i, _):
        v = i // 8
        m = pl.multiple_of(i % 8 * 16, 16)
        for h in range(2):
            lanes = slice(h * 128, h * 128 + 128)
            re = [hs[v, b, pl.ds(m, 16), lanes] for b in range(16)]
            im = [hs[v, b, pl.ds(m + 128, 16), lanes] for b in range(16)]
            re, im = dft(re, im)
            for q in range(16):
                a, b = re[q], im[q]
                if q:
                    a, b = rotated(a, b, tw[0, q : q + 1, lanes], tw[1, q : q + 1, lanes])
                hp[v, q, pl.ds(m, 16), lanes] = a.astype(BF16)
                hp[v, q, pl.ds(m + 128, 16), lanes] = b.astype(BF16)
        return 0

    lax.fori_loop(0, 16, strip, 0)
    def step_one(i):
        xo = (x + 2) % 4
        return (
            copy(pb.at[i, 0, xo], r1.at[i, 0], s1.at[i, 0], q1.at[i, 0], right),
            copy(pb.at[i, 1, xo], r1.at[i, 1], s1.at[i, 1], q1.at[i, 1], left),
        )

    def direct(i):
        return (
            copy(pb.at[i, 0, xm], rd.at[i, 0], sd.at[i, 0], qd.at[i, 0], left),
            copy(pb.at[i, 1, xp], rd.at[i, 1], sd.at[i, 1], qd.at[i, 1], right),
        )

    def forward(i):
        return (
            copy(fw.at[i, 0], rc.at[i, 0], sf.at[i, 0], qf.at[i, 0], right),
            copy(fw.at[i, 1], rc.at[i, 1], sf.at[i, 1], qf.at[i, 1], left),
        )

    def over(i):
        return copy(zb.at[i], zr.at[i], sz.at[i], qz.at[i], across)

    def compute(i):
        for q in range(4):
            rows = slice(q * 64, q * 64 + 64)
            part = None
            for v in range(2):
                h = hp[v, i]
                pc = lax.dot_general(dm[rows], h, NT, preferred_element_type=F32)
                ps = lax.dot_general(dm[256 + q * 64 : 320 + q * 64], h, NT, preferred_element_type=F32)
                dre = pc[:, :128] - ps[:, 128:]
                dim = ps[:, :128] + pc[:, 128:]
                term = eq[v, i, 0, rows] * dre - eq[v, i, 1, rows] * dim
                part = term if part is None else part + term
            for k in range(2):
                pb[i, q // 2, (q % 2) * 2 + k] = part[k * 32 : k * 32 + 32]

    def put(i, half, value):
        out_ref[pl.ds(half * 512 + i, 32, stride=16), :] = value

    lag1, lag2, lag3 = 4, 8, 12

    def turn(i, _):
        @pl.when(i < 16)
        def _():
            compute(i)
            for c in step_one(i) + direct(i):
                c.start()

        @pl.when(jnp.logical_and(i >= lag1, i < 16 + lag1))
        def _():
            j = i - lag1
            for c in step_one(j):
                c.wait_recv()
            fw[j, 0] = r1[j, 0] + pb[j, 0, xp]
            fw[j, 1] = r1[j, 1] + pb[j, 1, xm]
            for c in forward(j):
                c.start()

        @pl.when(jnp.logical_and(i >= lag2, i < 16 + lag2))
        def _():
            j = i - lag2
            for c in forward(j) + direct(j):
                c.wait_recv()
            put(j, zh, pb[j, zh, x] + rc[j, zh] + rd[j, zh])
            zb[j] = pb[j, 1 - zh, x] + rc[j, 1 - zh] + rd[j, 1 - zh]
            over(j).start()

        @pl.when(i >= lag3)
        def _():
            j = i - lag3
            over(j).wait_recv()
            put(j, 1 - zh, zr[j])

        return 0

    lax.fori_loop(0, 16 + lag3, turn, 0)

    def drain(i, _):
        for c in step_one(i) + direct(i) + forward(i) + (over(i),):
            c.wait_send()
        return 0

    lax.fori_loop(0, 16, drain, 0)
    for c in far:
        c.wait_send()
    for h in range(2):
        for g in range(4):
            swap(h, g).wait_send()


def local(visibility, target, offset, taps, w_plane):
    count = visibility.shape[1]
    dma = pltpu.SemaphoreType.DMA
    vmem = pl.BlockSpec(memory_space=pltpu.VMEM)
    smem = pl.BlockSpec(memory_space=pltpu.SMEM)
    buf = pltpu.VMEM((16, 2, 32, 128), F32)
    part = pltpu.VMEM((16, 32, 128), F32)
    halves = pl.pallas_call(
        kernel,
        out_shape=jax.ShapeDtypeStruct((1024, 128), F32),
        in_specs=[smem, smem] + [vmem] * 3,
        out_specs=vmem,
        scratch_shapes=[
            pltpu.VMEM((2, 4, 16, 128), F32),
            pltpu.VMEM((8, 128), F32),
            pltpu.VMEM((2, 8, 128), F32),
            pltpu.VMEM((4, 2, 16, 128), F32),
            pltpu.VMEM((3072, 128), F32),
            pltpu.VMEM((2, 16, 256, 256), F32),
            pltpu.VMEM((2, 16, 256, 256), BF16),
            pltpu.VMEM((2, 16, 2, 256, 128), F32),
            pltpu.VMEM((512, 256), BF16),
            pltpu.VMEM((2, 16, 256), F32),
            pltpu.VMEM((4, 4, 64, 128), F32),
            pltpu.VMEM((4, 8, 128), F32),
            pltpu.VMEM((4, 8, 128), F32),
            pltpu.VMEM((256, 128), F32),
            pltpu.VMEM((256, 128), F32),
            pltpu.VMEM((16, 2, 4, 32, 128), F32),
            buf,
            buf,
            buf,
            buf,
            part,
            part,
        ]
        + [dma((3,))] * 2
        + [dma((2, 3))] * 2
        + [dma((2, 4))] * 4
        + [dma] * 2
        + [dma((16, 2))] * 6
        + [dma((16,))] * 2,
        compiler_params=pltpu.CompilerParams(collective_id=0, has_side_effects=True, vmem_limit_bytes=56 << 20),
        name="dirtyimage",
    )(w_plane, taps, visibility, target.reshape(1, count), offset.reshape(1, count))
    return jnp.concatenate([halves[:512], halves[512:]], axis=1)


def solution(mesh):
    both = ("plane", "tile")
    return jax.shard_map(
        local,
        mesh=mesh,
        in_specs=(P(None, both), P(both, None), P(both), P(), P("plane")),
        out_specs=P("plane", "tile"),
        check_vma=False,
    )
```

```python
import math

import jax
import jax.numpy as jnp
from jax import lax
from jax.experimental import pallas as pl
from jax.experimental.pallas import tpu as pltpu
from jax.sharding import PartitionSpec as P


G = 4096
KS = 8
CHUNKS = 8
SUB = 16 // CHUNKS
MESH = pl.DeviceIdType.MESH
F32 = jnp.float32
BF16 = jnp.bfloat16
NT = (((1,), (1,)), ((), ()))

SIN = (3.1415927410125732, -5.167710304260254, 2.550077438354492, -0.598291277885437, 0.07765766233205795)
COS = (0.9999999403953552, -4.934792995452881, 4.058411121368408, -1.331876516342163, 0.21968960762023926)


def poly(coefs, g):
    out = g * coefs[-1] + coefs[-2]
    for c in coefs[-3::-1]:
        out = out * g + c
    return out


def cos_sin(cycles):
    f = cycles - jnp.floor(cycles + 0.5)
    g = f * f
    s = f * poly(SIN, g)
    c = poly(COS, g)
    s2 = s + s
    return 1.0 - s2 * s, s2 * c


def rotated(re, im, c, s):
    return re * c - im * s, re * s + im * c


def dft(re, im):
    n = len(re)
    if n == 1:
        return re, im
    er, ei = dft(re[0::2], im[0::2])
    dr, di = dft(re[1::2], im[1::2])
    h = n // 2
    out_r, out_i = [None] * n, [None] * n
    for k in range(h):
        if k == 0:
            tr, ti = dr[k], di[k]
        elif 4 * k == n:
            tr, ti = -di[k], dr[k]
        elif 8 * k == n:
            q = math.sqrt(0.5)
            tr, ti = (dr[k] - di[k]) * q, (dr[k] + di[k]) * q
        elif 8 * k == 3 * n:
            q = math.sqrt(0.5)
            tr, ti = (dr[k] + di[k]) * -q, (dr[k] - di[k]) * q
        else:
            c, s = math.cos(2 * math.pi * k / n), math.sin(2 * math.pi * k / n)
            tr, ti = dr[k] * c - di[k] * s, dr[k] * s + di[k] * c
        out_r[k], out_i[k] = er[k] + tr, ei[k] + ti
        out_r[k + h], out_i[k + h] = er[k] - tr, ei[k] - ti
    return out_r, out_i


def sort(vis_ref, tgt_ref, off_ref, out_ref):
    count = tgt_ref.shape[1]
    blk = 256
    ii = lax.broadcasted_iota(jnp.int32, (blk, blk), 0)
    jj = lax.broadcasted_iota(jnp.int32, (blk, blk), 1)
    tri = jnp.where(ii < jj, 1.0, 0.0).astype(BF16)
    rows = lax.broadcasted_iota(jnp.int32, (128, blk), 0)
    ranks = lax.broadcasted_iota(jnp.int32, (32, blk), 0).astype(F32)
    carry = jnp.zeros((128, 1), F32)
    acc = jnp.zeros((128, 128), F32)
    for b in range(count // blk):
        sl = slice(b * blk, (b + 1) * blk)
        one = jnp.where(rows == tgt_ref[:, sl], 1.0, 0.0)
        oneb = one.astype(BF16)
        before = jnp.dot(oneb, tri, preferred_element_type=F32)
        rank = jnp.sum(one * (before + carry), axis=0, keepdims=True)
        carry = carry + jnp.sum(one, axis=1, keepdims=True)
        hit = ranks == rank
        off = off_ref[:, sl]
        parts = [((off >> 12) << 12).astype(F32), (((off >> 4) & 255) << 4).astype(F32), (off & 15).astype(F32)]
        left = [vis_ref[0:1, sl], vis_ref[1:2, sl]]
        for k in range(3):
            cols = []
            for v in range(2):
                top = left[v].astype(BF16).astype(F32)
                left[v] = left[v] - top
                cols.append(jnp.where(hit, top, 0.0))
            cols.append(jnp.where(hit, parts[k], 0.0))
            cols.append(jnp.zeros((32, blk), F32))
            table = jnp.concatenate(cols, axis=0).astype(BF16)
            acc = acc + lax.dot_general(oneb, table, NT, preferred_element_type=F32)
    for q in range(8):
        out_ref[q // 4, q % 4] = acc[q * 16 : q * 16 + 16]


def place():
    p = lax.axis_index("plane")
    t = lax.axis_index("tile")
    return p // 4, p % 4, t // 8, (t // 2) % 4, t % 2


def kernel(w_ref, taps_ref, vis_ref, tgt_ref, off_ref, out_ref, *scratch):
    sb, wb, wo, ra, ga, hs, hp, eq, dm, tw, xs, ts, rs, sr, si, pb, r1, fw, rc, zb, zr, oh = scratch[:22]
    sa, qa, sn, qn, sv, qv, sc, qc, sw, qw, s1, q1, sf, qf, sz, qz = scratch[22:]
    zh, x, zl, y, core = place()
    z = zh * 2 + zl
    p, t = zh * 4 + x, zl * 8 + y * 2 + core
    xp, xm = (x + 1) % 4, (x + 3) % 4

    def at_x(d):
        return {"plane": zh * 4 + (x + d) % 4, "tile": t}

    def at_y(d):
        return {"plane": p, "tile": zl * 8 + ((y + d) % 4) * 2 + core}

    def at_z(d):
        zz = (z + d) % 4
        return {"plane": (zz // 2) * 4 + x, "tile": (zz % 2) * 8 + y * 2 + core}

    partner = {"plane": p, "tile": zl * 8 + y * 2 + (1 - core)}
    right, left, across = at_x(1), at_x(3), at_z(2)

    barrier = pltpu.get_barrier_semaphore()
    for d in (1, 2, 3):
        for at in (at_x, at_y, at_z):
            pl.semaphore_signal(barrier, inc=1, device_id=at(d), device_id_type=MESH)
    pl.semaphore_signal(barrier, inc=1, device_id=partner, device_id_type=MESH)

    def copy(src, dst, send, recv, device):
        return pltpu.make_async_remote_copy(
            src_ref=src, dst_ref=dst, send_sem=send, recv_sem=recv, device_id=device, device_id_type=MESH
        )

    sort(vis_ref, tgt_ref, off_ref, sb)
    wb[...] = jnp.full((8, 128), w_ref[0])
    wo[zh] = wb[...]
    pl.semaphore_wait(barrier, 10)
    first = [copy(sb.at[:, (x + d) % 4], ra.at[x], sa.at[d - 1], qa.at[d - 1], at_x(d)) for d in (1, 3, 2)]
    for c in first:
        c.start()
    wcopy = copy(wb, wo.at[zh], sw, qw, across)
    wcopy.start()
    ra[x] = sb[:, x]

    l0 = lax.broadcasted_iota(jnp.int32, (256, 128), 0)
    lane = lax.broadcasted_iota(jnp.int32, (256, 128), 1)
    ec, es = cos_sin((l0 * 16 + lane).astype(F32) * (1.0 / G))
    ar, ai = jnp.full((256, 128), taps_ref[KS - 1]), jnp.zeros((256, 128), F32)
    for j in range(KS - 2, -1, -1):
        ar, ai = rotated(ar, ai, ec, es)
        ar = ar + taps_ref[j]
    sr[...] = ar
    si[...] = ai
    m = t * 256 + zh * 128 + lax.broadcasted_iota(jnp.int32, (8, 128), 1)
    ec, es = cos_sin(m.astype(F32) * (1.0 / G))
    taps_low = [jnp.full((8, 128), taps_ref[j]).astype(BF16).astype(F32) for j in range(KS)]
    tr, ti = taps_low[KS - 1], jnp.zeros((8, 128), F32)
    for j in range(KS - 2, -1, -1):
        tr, ti = rotated(tr, ti, ec, es)
        tr = tr + taps_low[j]
    tr, ti = tr[0:1] * (1.0 / 512.0), ti[0:1] * (1.0 / 512.0)
    ym = jnp.where(m >= G // 2, m - G, m).astype(F32)[0:1] * (0.5 / G)
    ysq = ym * ym
    row64 = lax.broadcasted_iota(jnp.int32, (64, 128), 0)
    lane64 = lax.broadcasted_iota(jnp.int32, (64, 128), 1)

    def screen(n, _):
        v = jnp.where(n < 16, zh, 1 - zh)
        i = n % 16
        w = wo[v, 0:1, :]
        for q in range(4):
            rows = slice(q * 64, q * 64 + 64)
            l = (row64 + q * 64) * 16 + i
            xl = jnp.where(l >= G // 2, l - G, l).astype(F32) * (0.5 / G)
            rho = xl * xl + ysq
            n_minus = -rho / (1.0 + jnp.sqrt(1.0 - rho))
            c, s = cos_sin(w * n_minus)
            c, s = rotated(c, s, tr, ti)
            cs = jnp.sum(jnp.where(lane64 == i, sr[rows], 0.0), axis=1, keepdims=True)
            ss = jnp.sum(jnp.where(lane64 == i, si[rows], 0.0), axis=1, keepdims=True)
            c, s = rotated(c, s, cs, ss)
            eq[v, i, 0, rows] = c
            eq[v, i, 1, rows] = s
        return 0

    lax.fori_loop(0, 10, screen, 0)
    for c in first:
        c.wait()

    outer, inner = (z, y), (y, z)
    around = ((at_y, at_z), (at_z, at_y))

    def rows_of(h, g, cr):
        step = jnp.where(g == 0, 0, jnp.where(g == 1, 3, g - 1))
        o = (outer[h] + step) % 4
        return ga.at[pl.ds(pl.multiple_of(h * 1536 + (o * 2 + cr) * 192, 192), 192)]

    got = [ra[s].reshape(32, 128) for s in range(4)]
    group = lax.broadcasted_iota(jnp.int32, (32, 128), 1) // 32
    base = [pl.multiple_of(h * 1536 + ((outer[h] * 2 + core) * 4 + inner[h]) * 48, 48) for h in range(2)]
    for k in range(3):
        row = jnp.zeros((32, 128), F32)
        for s in range(4):
            shift = (32 * (s - k)) % 128
            moved = pltpu.roll(got[s], shift, 1) if shift else got[s]
            row = jnp.where(group == s, moved, row)
        for h in range(2):
            ga[pl.ds(base[h] + k * 16, 16)] = row[h * 16 : h * 16 + 16]
    near = []
    for d in (1, 3, 2):
        for h in range(2):
            mine = ga.at[pl.ds(base[h], 48)]
            near.append(copy(mine, mine, sn.at[h, d - 1], qn.at[h, d - 1], around[h][0](d)))
    for c in near:
        c.start()
    wcopy.wait()
    lax.fori_loop(10, 20, screen, 0)
    for q in range(8):
        a = lax.broadcasted_iota(jnp.int32, (32, 256), 0) + q * 32
        b = lax.broadcasted_iota(jnp.int32, (32, 256), 1)
        c, s = cos_sin(((a * b) % 256).astype(F32) * (1.0 / 256.0))
        dm[q * 32 : q * 32 + 32] = c.astype(BF16)
        dm[256 + q * 32 : 288 + q * 32] = s.astype(BF16)
    a = lax.broadcasted_iota(jnp.int32, (16, 256), 0)
    b = lax.broadcasted_iota(jnp.int32, (16, 256), 1)
    c, s = cos_sin((a * b).astype(F32) * (1.0 / G))
    tw[0] = c
    tw[1] = s
    for c in near:
        c.wait()

    far = []
    for g, d in ((1, 1), (2, 3), (3, 2)):
        for h in range(2):
            own = rows_of(h, 0, core)
            far.append(copy(own, own, sv.at[h, g], qv.at[h, g], around[h][1](d)))

    def arrival(h, g):
        part = rows_of(h, g, core)
        return copy(part, part, sv.at[h, g], qv.at[h, g], across)

    def swap(h, g):
        part = rows_of(h, g, core)
        return copy(part, part, sc.at[h, g], qc.at[h, g], partner)

    def swapped(h, g):
        part = rows_of(h, g, 1 - core)
        return copy(part, part, sc.at[h, g], qc.at[h, g], partner)

    for h in range(2):
        swap(h, 0).start()
    for c in far:
        c.start()

    mb = (t * 256 + zh * 128).astype(F32)
    sub = lax.broadcasted_iota(jnp.int32, (8, 128), 0).astype(F32)

    def start_of(h, g):
        step = jnp.where(g == 0, 0, jnp.where(g == 1, 3, g - 1))
        o = (jnp.where(h == 0, outer[0], outer[1]) + step) % 4
        return h * 1536 + o * 384

    def dense(start, u):
        re = ga[pl.ds(start, 8, stride=48), :]
        im = ga[pl.ds(start + 16, 8, stride=48), :]
        off = ga[pl.ds(start + 32, 8, stride=48), :]
        row = jnp.floor(off * (1.0 / G))
        col = off - row * G
        cb, sb_ = cos_sin(col * mb * (1.0 / G))
        c1, s1_ = cos_sin(col * (1.0 / G))
        c8, s8 = cos_sin(col * (8.0 / G))
        re, im = rotated(re, im, cb, sb_)
        for s in range(8):
            nr, ni = rotated(re, im, c8, s8)
            xs[u, 0, s * 8 : s * 8 + 8] = re
            xs[u, 1, s * 8 : s * 8 + 8] = im
            xs[u, 2, s * 8 : s * 8 + 8] = nr
            xs[u, 3, s * 8 : s * 8 + 8] = ni
            if s < 7:
                re, im = rotated(re, im, c1, s1_)
        ts[u] = c8 + c8
        rs[u] = row

    def product(u):
        tabs, hots = [], []
        for dev in range(8):
            turn = jnp.broadcast_to(ts[u, dev : dev + 1, :], (8, 128))
            rows = []
            for v in range(2):
                a = xs[u, v, pl.ds(dev, 8, stride=8), :]
                b = xs[u, 2 + v, pl.ds(dev, 8, stride=8), :]
                for k in range(16):
                    rows.append(a)
                    a, b = b, turn * b - a
            tabs.append(jnp.concatenate(rows, axis=0))
            r = jnp.broadcast_to(rs[u, dev : dev + 1, :], (8, 128)) - sub
            hots.append(jnp.concatenate([jnp.where(r == 8.0 * j, 1.0, 0.0) for j in range(32)], axis=0))
        return tabs, hots

    def total(us):
        tabs, hots = [], []
        for u in us:
            a, b = product(u)
            tabs += a
            hots += b
        tab, hot = jnp.concatenate(tabs, axis=1), jnp.concatenate(hots, axis=1)
        return lax.dot_general(tab, hot, NT, preferred_element_type=F32)

    def early(h, _):
        start = start_of(h, 0)

        def quad(it, _):
            for u in range(4):
                dense(start + it * 4 + u, u)
            for u in range(4):
                hs[h, it * 4 + u] = total([u])
            return 0

        lax.fori_loop(0, 4, quad, 0)
        return 0

    for h in range(2):
        swapped(h, 0).wait_recv()
    lax.fori_loop(0, 2, early, 0)
    for g in (1, 2):
        for h in range(2):
            arrival(h, g).wait_recv()
            swap(h, g).start()
    lax.fori_loop(20, 25, screen, 0)
    for h in range(2):
        arrival(h, 3).wait_recv()
        swap(h, 3).start()
    lax.fori_loop(25, 32, screen, 0)
    for g in (1, 2, 3):
        for h in range(2):
            swapped(h, g).wait_recv()

    def late(h, _):
        starts = [start_of(h, g) for g in (1, 2, 3)]
        for u in range(3):
            dense(starts[u], u)

        def one(band, _):
            hs[h, band] += total([0, 1, 2])
            following = jnp.minimum(band + 1, 15)
            for u in range(3):
                dense(starts[u] + following, u)
            return 0

        lax.fori_loop(0, 16, one, 0)
        return 0

    lax.fori_loop(0, 2, late, 0)

    def strip(i, _):
        v = i // 8
        m = pl.multiple_of(i % 8 * 16, 16)
        for h in range(2):
            lanes = slice(h * 128, h * 128 + 128)
            re = [hs[v, b, pl.ds(m, 16), lanes] for b in range(16)]
            im = [hs[v, b, pl.ds(m + 128, 16), lanes] for b in range(16)]
            re, im = dft(re, im)
            for q in range(16):
                a, b = re[q], im[q]
                if q:
                    a, b = rotated(a, b, tw[0, q : q + 1, lanes], tw[1, q : q + 1, lanes])
                hp[v, q, pl.ds(m, 16), lanes] = a.astype(BF16)
                hp[v, q, pl.ds(m + 128, 16), lanes] = b.astype(BF16)
        return 0

    lax.fori_loop(0, 16, strip, 0)
    def step_one(i):
        xo = (x + 2) % 4
        return (
            copy(pb.at[i, 0, xo], r1.at[i, 0], s1, q1.at[i, 0], right),
            copy(pb.at[i, 1, xo], r1.at[i, 1], s1, q1.at[i, 1], left),
        )

    def step_two(i):
        return (
            copy(fw.at[i, 0], rc.at[i, 0], sf, qf.at[i, 0], right),
            copy(fw.at[i, 1], rc.at[i, 1], sf, qf.at[i, 1], left),
        )

    def over(i):
        return copy(zb.at[i], zr.at[i], sz, qz.at[i], across)

    def compute(i):
        for k in range(SUB):
            j = i * SUB + k
            pair = [lax.dot_general(dm[...], hp[v, j], NT, preferred_element_type=F32) for v in range(2)]
            for q in range(8):
                rows = slice(q * 32, q * 32 + 32)
                part = None
                for v in range(2):
                    pc, ps = pair[v][q * 32 : q * 32 + 32], pair[v][256 + q * 32 : 288 + q * 32]
                    dre = pc[:, :128] - ps[:, 128:]
                    dim = ps[:, :128] + pc[:, 128:]
                    term = eq[v, j, 0, rows] * dre - eq[v, j, 1, rows] * dim
                    part = term if part is None else part + term
                pb[i, q // 4, q % 4, k] = part

    def put(i, half, value):
        for k in range(SUB):
            oh[pl.ds(half * 512 + i * SUB + k, 32, stride=16), :] = value[k]

    lag1, lag2, lag3 = 4, 7, 9

    def turn(i, _):
        @pl.when(i < CHUNKS)
        def _():
            compute(i)
            for c in step_one(i):
                c.start()

        @pl.when(jnp.logical_and(i >= lag1, i < CHUNKS + lag1))
        def _():
            j = i - lag1
            for c in step_one(j):
                c.wait_recv()
            fw[j, 0, 0] = r1[j, 0] + pb[j, 0, xp]
            fw[j, 0, 1] = pb[j, 1, xp]
            fw[j, 1, 0] = pb[j, 0, xm]
            fw[j, 1, 1] = r1[j, 1] + pb[j, 1, xm]
            for c in step_two(j):
                c.start()

        @pl.when(jnp.logical_and(i >= lag2, i < CHUNKS + lag2))
        def _():
            j = i - lag2
            for c in step_two(j):
                c.wait_recv()
            zb[j] = pb[j, 1 - zh, x] + rc[j, 0, 1 - zh] + rc[j, 1, 1 - zh]
            over(j).start()
            put(j, zh, pb[j, zh, x] + rc[j, 0, zh] + rc[j, 1, zh])

        @pl.when(i >= lag3)
        def _():
            j = i - lag3
            over(j).wait_recv()
            put(j, 1 - zh, zr[j])

        return 0

    lax.fori_loop(0, CHUNKS + lag3, turn, 0)
    out_ref[:, :128] = oh[:512]
    out_ref[:, 128:] = oh[512:]
    copy(r1, r1, s1, q1.at[0, 0], right).wait_send()
    copy(fw, fw, sf, qf.at[0, 0], right).wait_send()
    copy(zb, zb, sz, qz.at[0], right).wait_send()
    for c in far:
        c.wait_send()
    for h in range(2):
        for g in range(4):
            swap(h, g).wait_send()


def local(visibility, target, offset, taps, w_plane):
    count = visibility.shape[1]
    dma = pltpu.SemaphoreType.DMA
    vmem = pl.BlockSpec(memory_space=pltpu.VMEM)
    smem = pl.BlockSpec(memory_space=pltpu.SMEM)
    pair = pltpu.VMEM((CHUNKS, 2, 2, SUB, 32, 128), F32)
    part = pltpu.VMEM((CHUNKS, SUB, 32, 128), F32)
    return pl.pallas_call(
        kernel,
        out_shape=jax.ShapeDtypeStruct((512, 256), F32),
        in_specs=[smem, smem] + [vmem] * 3,
        out_specs=vmem,
        scratch_shapes=[
            pltpu.VMEM((2, 4, 16, 128), F32),
            pltpu.VMEM((8, 128), F32),
            pltpu.VMEM((2, 8, 128), F32),
            pltpu.VMEM((4, 2, 16, 128), F32),
            pltpu.VMEM((3072, 128), F32),
            pltpu.VMEM((2, 16, 256, 256), F32),
            pltpu.VMEM((2, 16, 256, 256), BF16),
            pltpu.VMEM((2, 16, 2, 256, 128), F32),
            pltpu.VMEM((512, 256), BF16),
            pltpu.VMEM((2, 16, 256), F32),
            pltpu.VMEM((4, 4, 64, 128), F32),
            pltpu.VMEM((4, 8, 128), F32),
            pltpu.VMEM((4, 8, 128), F32),
            pltpu.VMEM((256, 128), F32),
            pltpu.VMEM((256, 128), F32),
            pltpu.VMEM((CHUNKS, 2, 4, SUB, 32, 128), F32),
            pltpu.VMEM((CHUNKS, 2, SUB, 32, 128), F32),
            pair,
            pair,
            part,
            part,
            pltpu.VMEM((1024, 128), F32),
        ]
        + [dma((3,))] * 2
        + [dma((2, 3))] * 2
        + [dma((2, 4))] * 4
        + [dma] * 3
        + [dma((CHUNKS, 2)), dma] * 2
        + [dma((CHUNKS,))],
        compiler_params=pltpu.CompilerParams(collective_id=0, has_side_effects=True, vmem_limit_bytes=56 << 20),
        name="dirtyimage",
    )(w_plane, taps, visibility, target.reshape(1, count), offset.reshape(1, count))


def solution(mesh):
    both = ("plane", "tile")
    return jax.shard_map(
        local,
        mesh=mesh,
        in_specs=(P(None, both), P(both, None), P(both), P(), P("plane")),
        out_specs=P("plane", "tile"),
        check_vma=False,
    )
```

```python
import math

import jax
import jax.numpy as jnp
from jax import lax
from jax.experimental import pallas as pl
from jax.experimental.pallas import tpu as pltpu
from jax.sharding import PartitionSpec as P


G = 4096
KS = 8
CHUNKS, SUB = 8, 2
MESH = pl.DeviceIdType.MESH
F32 = jnp.float32
BF16 = jnp.bfloat16
NT = (((1,), (1,)), ((), ()))

SIN = (3.1415927410125732, -5.167710304260254, 2.550077438354492, -0.598291277885437, 0.07765766233205795)
COS = (0.9999999403953552, -4.934792995452881, 4.058411121368408, -1.331876516342163, 0.21968960762023926)


def poly(coefs, g):
    out = g * coefs[-1] + coefs[-2]
    for c in coefs[-3::-1]:
        out = out * g + c
    return out


def cos_sin(cycles):
    f = cycles - jnp.floor(cycles + 0.5)
    g = f * f
    s = f * poly(SIN, g)
    c = poly(COS, g)
    s2 = s + s
    return 1.0 - s2 * s, s2 * c


def rotated(re, im, c, s):
    return re * c - im * s, re * s + im * c


def dft(re, im):
    n = len(re)
    if n == 1:
        return re, im
    er, ei = dft(re[0::2], im[0::2])
    dr, di = dft(re[1::2], im[1::2])
    h = n // 2
    out_r, out_i = [None] * n, [None] * n
    for k in range(h):
        if k == 0:
            tr, ti = dr[k], di[k]
        elif 4 * k == n:
            tr, ti = -di[k], dr[k]
        elif 8 * k == n:
            q = math.sqrt(0.5)
            tr, ti = (dr[k] - di[k]) * q, (dr[k] + di[k]) * q
        elif 8 * k == 3 * n:
            q = math.sqrt(0.5)
            tr, ti = (dr[k] + di[k]) * -q, (dr[k] - di[k]) * q
        else:
            c, s = math.cos(2 * math.pi * k / n), math.sin(2 * math.pi * k / n)
            tr, ti = dr[k] * c - di[k] * s, dr[k] * s + di[k] * c
        out_r[k], out_i[k] = er[k] + tr, ei[k] + ti
        out_r[k + h], out_i[k + h] = er[k] - tr, ei[k] - ti
    return out_r, out_i


def sort(in_ref, out_ref):
    count = in_ref.shape[1]
    blk = 256
    ii = lax.broadcasted_iota(jnp.int32, (blk, blk), 0)
    jj = lax.broadcasted_iota(jnp.int32, (blk, blk), 1)
    tri = jnp.where(ii < jj, 1.0, 0.0).astype(BF16)
    rows = lax.broadcasted_iota(jnp.int32, (128, blk), 0).astype(F32)
    ranks = lax.broadcasted_iota(jnp.int32, (32, blk), 0).astype(F32)
    carry = jnp.zeros((128, 1), F32)
    acc = jnp.zeros((128, 128), F32)
    for b in range(count // blk):
        sl = slice(b * blk, (b + 1) * blk)
        one = jnp.where(rows == in_ref[2:3, sl], 1.0, 0.0)
        oneb = one.astype(BF16)
        before = jnp.dot(oneb, tri, preferred_element_type=F32)
        rank = jnp.sum(one * (before + carry), axis=0, keepdims=True)
        carry = carry + jnp.sum(one, axis=1, keepdims=True)
        hit = ranks == rank
        off = in_ref[3:4, sl]
        high = jnp.floor(off * (1.0 / 4096.0)) * 4096.0
        mid = jnp.floor((off - high) * (1.0 / 16.0)) * 16.0
        parts = [high, mid, off - high - mid]
        left = [in_ref[0:1, sl], in_ref[1:2, sl]]
        for k in range(3):
            cols = []
            for v in range(2):
                top = left[v].astype(BF16).astype(F32)
                left[v] = left[v] - top
                cols.append(jnp.where(hit, top, 0.0))
            cols.append(jnp.where(hit, parts[k], 0.0))
            cols.append(jnp.zeros((32, blk), F32))
            table = jnp.concatenate(cols, axis=0).astype(BF16)
            acc = acc + lax.dot_general(oneb, table, NT, preferred_element_type=F32)
    for q in range(8):
        out_ref[q // 4, q % 4] = acc[q * 16 : q * 16 + 16]


def place():
    p = lax.axis_index("plane")
    t = lax.axis_index("tile")
    return p // 4, p % 4, t // 8, (t // 2) % 4, t % 2


def kernel(in_ref, out_ref, *scratch):
    sb, wb, wo, ra, ga, hs, hp, eq, dm, tw, xs, ts, rs, sr, si, pb, r1, fw, rc, zb, zr, oh = scratch[:22]
    sa, qa, sn, qn, sv, qv, sc, qc, sw, qw, s1, q1, sf, qf, sz, qz = scratch[22:]
    zh, x, zl, y, core = place()
    z = zh * 2 + zl
    p, t = zh * 4 + x, zl * 8 + y * 2 + core
    xp, xm = (x + 1) % 4, (x + 3) % 4

    def at_x(d):
        return {"plane": zh * 4 + (x + d) % 4, "tile": t}

    def at_y(d):
        return {"plane": p, "tile": zl * 8 + ((y + d) % 4) * 2 + core}

    def at_z(d):
        zz = (z + d) % 4
        return {"plane": (zz // 2) * 4 + x, "tile": (zz % 2) * 8 + y * 2 + core}

    partner = {"plane": p, "tile": zl * 8 + y * 2 + (1 - core)}
    right, left, across = at_x(1), at_x(3), at_z(2)

    barrier = pltpu.get_barrier_semaphore()
    for d in (1, 2, 3):
        for at in (at_x, at_y, at_z):
            pl.semaphore_signal(barrier, inc=1, device_id=at(d), device_id_type=MESH)
    pl.semaphore_signal(barrier, inc=1, device_id=partner, device_id_type=MESH)

    def copy(src, dst, send, recv, device):
        return pltpu.make_async_remote_copy(
            src_ref=src, dst_ref=dst, send_sem=send, recv_sem=recv, device_id=device, device_id_type=MESH
        )

    for q in range(8):
        a = lax.broadcasted_iota(jnp.int32, (32, 256), 0) + q * 32
        b = lax.broadcasted_iota(jnp.int32, (32, 256), 1)
        c, s = cos_sin(((a * b) % 256).astype(F32) * (1.0 / 256.0))
        dm[q * 32 : q * 32 + 32] = c.astype(BF16)
        dm[256 + q * 32 : 288 + q * 32] = s.astype(BF16)
    a = lax.broadcasted_iota(jnp.int32, (16, 256), 0)
    b = lax.broadcasted_iota(jnp.int32, (16, 256), 1)
    c, s = cos_sin((a * b).astype(F32) * (1.0 / G))
    tw[0] = c
    tw[1] = s
    sort(in_ref, sb)
    small = in_ref[4:5, 0:128]

    def spread(n, shape):
        return jnp.broadcast_to(small[:, n : n + 1], shape)

    wb[...] = spread(KS, (8, 128))
    wo[zh] = wb[...]
    pl.semaphore_wait(barrier, 10)
    first = [copy(sb.at[:, (x + d) % 4], ra.at[x], sa.at[d - 1], qa.at[d - 1], at_x(d)) for d in (1, 3, 2)]
    for c in first:
        c.start()
    wcopy = copy(wb, wo.at[zh], sw, qw, across)
    wcopy.start()
    ra[x] = sb[:, x]

    l0 = lax.broadcasted_iota(jnp.int32, (256, 128), 0)
    lane = lax.broadcasted_iota(jnp.int32, (256, 128), 1)
    ec, es = cos_sin((l0 * 16 + lane).astype(F32) * (1.0 / G))
    ar, ai = spread(KS - 1, (256, 128)), jnp.zeros((256, 128), F32)
    for j in range(KS - 2, -1, -1):
        ar, ai = rotated(ar, ai, ec, es)
        ar = ar + spread(j, (256, 128))
    sr[...] = ar
    si[...] = ai
    m = t * 256 + zh * 128 + lax.broadcasted_iota(jnp.int32, (8, 128), 1)
    ec, es = cos_sin(m.astype(F32) * (1.0 / G))
    taps_low = [spread(j, (8, 128)).astype(BF16).astype(F32) for j in range(KS)]
    tr, ti = taps_low[KS - 1], jnp.zeros((8, 128), F32)
    for j in range(KS - 2, -1, -1):
        tr, ti = rotated(tr, ti, ec, es)
        tr = tr + taps_low[j]
    tr, ti = tr[0:1] * (1.0 / 512.0), ti[0:1] * (1.0 / 512.0)
    ym = jnp.where(m >= G // 2, m - G, m).astype(F32)[0:1] * (0.5 / G)
    ysq = ym * ym
    row64 = lax.broadcasted_iota(jnp.int32, (64, 128), 0)
    lane64 = lax.broadcasted_iota(jnp.int32, (64, 128), 1)

    def screen(n, _):
        v = jnp.where(n < 16, zh, 1 - zh)
        i = n % 16
        w = wo[v, 0:1, :]
        for q in range(4):
            rows = slice(q * 64, q * 64 + 64)
            l = (row64 + q * 64) * 16 + i
            xl = jnp.where(l >= G // 2, l - G, l).astype(F32) * (0.5 / G)
            rho = xl * xl + ysq
            n_minus = -rho / (1.0 + jnp.sqrt(1.0 - rho))
            c, s = cos_sin(w * n_minus)
            c, s = rotated(c, s, tr, ti)
            cs = jnp.sum(jnp.where(lane64 == i, sr[rows], 0.0), axis=1, keepdims=True)
            ss = jnp.sum(jnp.where(lane64 == i, si[rows], 0.0), axis=1, keepdims=True)
            c, s = rotated(c, s, cs, ss)
            eq[v, i, 0, rows] = c
            eq[v, i, 1, rows] = s
        return 0

    lax.fori_loop(0, 13, screen, 0)
    for c in first:
        c.wait()

    outer, inner = (z, y), (y, z)
    around = ((at_y, at_z), (at_z, at_y))

    def rows_of(h, g, cr):
        step = jnp.where(g == 0, 0, jnp.where(g == 1, 3, g - 1))
        o = (outer[h] + step) % 4
        return ga.at[pl.ds(pl.multiple_of(h * 1536 + (o * 2 + cr) * 192, 192), 192)]

    got = [ra[s].reshape(32, 128) for s in range(4)]
    group = lax.broadcasted_iota(jnp.int32, (32, 128), 1) // 32
    base = [pl.multiple_of(h * 1536 + ((outer[h] * 2 + core) * 4 + inner[h]) * 48, 48) for h in range(2)]
    for k in range(3):
        row = jnp.zeros((32, 128), F32)
        for s in range(4):
            shift = (32 * (s - k)) % 128
            moved = pltpu.roll(got[s], shift, 1) if shift else got[s]
            row = jnp.where(group == s, moved, row)
        for h in range(2):
            ga[pl.ds(base[h] + k * 16, 16)] = row[h * 16 : h * 16 + 16]
    near = []
    for d in (1, 3, 2):
        for h in range(2):
            mine = ga.at[pl.ds(base[h], 48)]
            near.append(copy(mine, mine, sn.at[h, d - 1], qn.at[h, d - 1], around[h][0](d)))
    for c in near:
        c.start()
    wcopy.wait()
    lax.fori_loop(13, 28, screen, 0)
    for c in near:
        c.wait()

    far = []
    for g, d in ((1, 1), (2, 3), (3, 2)):
        for h in range(2):
            own = rows_of(h, 0, core)
            far.append(copy(own, own, sv.at[h, g], qv.at[h, g], around[h][1](d)))

    def arrival(h, g):
        part = rows_of(h, g, core)
        return copy(part, part, sv.at[h, g], qv.at[h, g], across)

    def swap(h, g):
        part = rows_of(h, g, core)
        return copy(part, part, sc.at[h, g], qc.at[h, g], partner)

    def swapped(h, g):
        part = rows_of(h, g, 1 - core)
        return copy(part, part, sc.at[h, g], qc.at[h, g], partner)

    for h in range(2):
        swap(h, 0).start()
    for c in far:
        c.start()

    mb = (t * 256 + zh * 128).astype(F32)
    sub = lax.broadcasted_iota(jnp.int32, (8, 128), 0).astype(F32)

    def start_of(h, g):
        step = jnp.where(g == 0, 0, jnp.where(g == 1, 3, g - 1))
        o = (jnp.where(h == 0, outer[0], outer[1]) + step) % 4
        return h * 1536 + o * 384

    def dense(start, u):
        re = ga[pl.ds(start, 8, stride=48), :]
        im = ga[pl.ds(start + 16, 8, stride=48), :]
        off = ga[pl.ds(start + 32, 8, stride=48), :]
        row = jnp.floor(off * (1.0 / G))
        col = off - row * G
        cb, sb_ = cos_sin(col * mb * (1.0 / G))
        c1, s1_ = cos_sin(col * (1.0 / G))
        c8, s8 = cos_sin(col * (8.0 / G))
        re, im = rotated(re, im, cb, sb_)
        for s in range(8):
            nr, ni = rotated(re, im, c8, s8)
            xs[u, 0, s * 8 : s * 8 + 8] = re
            xs[u, 1, s * 8 : s * 8 + 8] = im
            xs[u, 2, s * 8 : s * 8 + 8] = nr
            xs[u, 3, s * 8 : s * 8 + 8] = ni
            if s < 7:
                re, im = rotated(re, im, c1, s1_)
        ts[u] = c8 + c8
        rs[u] = row

    def product(u):
        tabs, hots = [], []
        for dev in range(8):
            turn = jnp.broadcast_to(ts[u, dev : dev + 1, :], (8, 128))
            rows = []
            for v in range(2):
                a = xs[u, v, pl.ds(dev, 8, stride=8), :]
                b = xs[u, 2 + v, pl.ds(dev, 8, stride=8), :]
                for k in range(16):
                    rows.append(a)
                    a, b = b, turn * b - a
            tabs.append(jnp.concatenate(rows, axis=0))
            r = jnp.broadcast_to(rs[u, dev : dev + 1, :], (8, 128)) - sub
            hots.append(jnp.concatenate([jnp.where(r == 8.0 * j, 1.0, 0.0) for j in range(32)], axis=0))
        return tabs, hots

    def total(us):
        tabs, hots = [], []
        for u in us:
            a, b = product(u)
            tabs += a
            hots += b
        tab, hot = jnp.concatenate(tabs, axis=1), jnp.concatenate(hots, axis=1)
        return lax.dot_general(tab, hot, NT, preferred_element_type=F32)

    def fill(h, g, it):
        for u in range(4):
            dense(start_of(h, g) + it * 4 + u, u)

    def early(n, _):
        h, it = n // 4, n % 4
        fill(h, 0, it)
        for u in range(4):
            hs[h, it * 4 + u] = total([u])
        return 0

    for h in range(2):
        swapped(h, 0).wait_recv()
    lax.fori_loop(0, 8, early, 0)
    for h in range(2):
        arrival(h, 1).wait_recv()
        swap(h, 1).start()
    lax.fori_loop(28, 32, screen, 0)

    def late(n, _):
        g, h, it = 1 + n // 8, n // 4 % 2, n % 4

        @pl.when(n % 8 == 0)
        def _():
            for k in range(2):
                swapped(k, g).wait_recv()

        @pl.when(n == 3)
        def _():
            for f in (2, 3):
                for k in range(2):
                    arrival(k, f).wait_recv()
                    swap(k, f).start()

        fill(h, g, it)
        for u in range(4):
            hs[h, it * 4 + u] += total([u])
        return 0

    lax.fori_loop(0, 24, late, 0)

    def strip(rho):
        def some(i, _):
            v = i // 8
            m = pl.multiple_of(i % 8 * 16, 16)
            for h in range(2):
                lanes = slice(h * 128, h * 128 + 128)
                outs_r, outs_i = [], []
                for b in range(4):
                    r = [hs[v, b + 4 * k, pl.ds(m, 16), lanes] for k in range(4)]
                    q = [hs[v, b + 4 * k, pl.ds(m + 128, 16), lanes] for k in range(4)]
                    if rho % 2 == 0:
                        er, ei, dr, di = r[0] + r[2], q[0] + q[2], r[1] + r[3], q[1] + q[3]
                        yr, yi = (er + dr, ei + di) if rho == 0 else (er - dr, ei - di)
                    else:
                        er, ei, dr, di = r[0] - r[2], q[0] - q[2], r[1] - r[3], q[1] - q[3]
                        yr, yi = (er - di, ei + dr) if rho == 1 else (er + di, ei - dr)
                    if b and rho:
                        turn = 2 * math.pi * b * rho / 16
                        yr, yi = rotated(yr, yi, math.cos(turn), math.sin(turn))
                    outs_r.append(yr)
                    outs_i.append(yi)
                outs_r, outs_i = dft(outs_r, outs_i)
                for k in range(4):
                    c, d, j = outs_r[k], outs_i[k], rho + 4 * k
                    if j:
                        c, d = rotated(c, d, tw[0, j : j + 1, lanes], tw[1, j : j + 1, lanes])
                    hp[v, j, pl.ds(m, 16), lanes] = c.astype(BF16)
                    hp[v, j, pl.ds(m + 128, 16), lanes] = d.astype(BF16)
            return 0

        return some

    def row_class(i, k):
        return i // 2 + 4 * (i % 2 * 2 + k)

    def step_one(i):
        xo = (x + 2) % 4
        return (
            copy(pb.at[i, 0, xo], r1.at[i, 0], s1, q1.at[i, 0], right),
            copy(pb.at[i, 1, xo], r1.at[i, 1], s1, q1.at[i, 1], left),
        )

    def step_two(i):
        return (
            copy(fw.at[i, 0], rc.at[i, 0], sf, qf.at[i, 0], right),
            copy(fw.at[i, 1], rc.at[i, 1], sf, qf.at[i, 1], left),
        )

    def over(i):
        return copy(zb.at[i], zr.at[i], sz, qz.at[i], across)

    def compute(i):
        for k in range(SUB):
            j = row_class(i, k)
            pair = [lax.dot_general(dm[...], hp[v, j], NT, preferred_element_type=F32) for v in range(2)]
            for q in range(8):
                rows = slice(q * 32, q * 32 + 32)
                part = None
                for v in range(2):
                    pc, ps = pair[v][q * 32 : q * 32 + 32], pair[v][256 + q * 32 : 288 + q * 32]
                    dre = pc[:, :128] - ps[:, 128:]
                    dim = ps[:, :128] + pc[:, 128:]
                    term = eq[v, j, 0, rows] * dre - eq[v, j, 1, rows] * dim
                    part = term if part is None else part + term
                pb[i, q // 4, q % 4, k] = part

    def put(i, half, value):
        for k in range(SUB):
            oh[pl.ds(half * 512 + row_class(i, k), 32, stride=16), :] = value[k]

    lag1, lag2, lag3 = 2, 5, 7

    def turn(i, _):
        for rho in range(4):

            @pl.when(i == 2 * rho)
            def _():
                lax.fori_loop(0, 16, strip(rho), 0)

        @pl.when(i < CHUNKS)
        def _():
            compute(i)
            for c in step_one(i):
                c.start()

        @pl.when(jnp.logical_and(i >= lag1, i < CHUNKS + lag1))
        def _():
            j = i - lag1
            for c in step_one(j):
                c.wait_recv()
            fw[j, 0, 0] = r1[j, 0] + pb[j, 0, xp]
            fw[j, 0, 1] = pb[j, 1, xp]
            fw[j, 1, 0] = pb[j, 0, xm]
            fw[j, 1, 1] = r1[j, 1] + pb[j, 1, xm]
            for c in step_two(j):
                c.start()

        @pl.when(jnp.logical_and(i >= lag2, i < CHUNKS + lag2))
        def _():
            j = i - lag2
            for c in step_two(j):
                c.wait_recv()
            zb[j] = pb[j, 1 - zh, x] + rc[j, 0, 1 - zh] + rc[j, 1, 1 - zh]
            over(j).start()
            put(j, zh, pb[j, zh, x] + rc[j, 0, zh] + rc[j, 1, zh])

        @pl.when(i >= lag3)
        def _():
            j = i - lag3
            over(j).wait_recv()
            put(j, 1 - zh, zr[j])

        return 0

    lax.fori_loop(0, CHUNKS + lag3, turn, 0)
    out_ref[:, :128] = oh[:512]
    out_ref[:, 128:] = oh[512:]
    copy(r1, r1, s1, q1.at[0, 0], right).wait_send()
    copy(fw, fw, sf, qf.at[0, 0], right).wait_send()
    copy(zb, zb, sz, qz.at[0], right).wait_send()
    for c in far:
        c.wait_send()
    for h in range(2):
        for g in range(4):
            swap(h, g).wait_send()


def local(visibility, target, offset, taps, w_plane):
    count = visibility.shape[1]
    dma = pltpu.SemaphoreType.DMA
    vmem = pl.BlockSpec(memory_space=pltpu.VMEM)
    small = jnp.concatenate([taps, w_plane, jnp.zeros((count - KS - 1,), F32)])
    rows = [visibility, target.reshape(1, count).astype(F32), offset.reshape(1, count).astype(F32)]
    packed = jnp.concatenate(rows + [small.reshape(1, count), jnp.zeros((3, count), F32)], axis=0)
    pair = pltpu.VMEM((CHUNKS, 2, 2, SUB, 32, 128), F32)
    part = pltpu.VMEM((CHUNKS, SUB, 32, 128), F32)
    return pl.pallas_call(
        kernel,
        out_shape=jax.ShapeDtypeStruct((512, 256), F32),
        in_specs=[vmem],
        out_specs=vmem,
        scratch_shapes=[
            pltpu.VMEM((2, 4, 16, 128), F32),
            pltpu.VMEM((8, 128), F32),
            pltpu.VMEM((2, 8, 128), F32),
            pltpu.VMEM((4, 2, 16, 128), F32),
            pltpu.VMEM((3072, 128), F32),
            pltpu.VMEM((2, 16, 256, 256), F32),
            pltpu.VMEM((2, 16, 256, 256), BF16),
            pltpu.VMEM((2, 16, 2, 256, 128), F32),
            pltpu.VMEM((512, 256), BF16),
            pltpu.VMEM((2, 16, 256), F32),
            pltpu.VMEM((4, 4, 64, 128), F32),
            pltpu.VMEM((4, 8, 128), F32),
            pltpu.VMEM((4, 8, 128), F32),
            pltpu.VMEM((256, 128), F32),
            pltpu.VMEM((256, 128), F32),
            pltpu.VMEM((CHUNKS, 2, 4, SUB, 32, 128), F32),
            pltpu.VMEM((CHUNKS, 2, SUB, 32, 128), F32),
            pair,
            pair,
            part,
            part,
            pltpu.VMEM((1024, 128), F32),
        ]
        + [dma((3,))] * 2
        + [dma((2, 3))] * 2
        + [dma((2, 4))] * 4
        + [dma] * 3
        + [dma((CHUNKS, 2)), dma] * 2
        + [dma((CHUNKS,))],
        compiler_params=pltpu.CompilerParams(collective_id=0, has_side_effects=True, vmem_limit_bytes=36 << 20),
        name="dirtyimage",
    )(packed)


def solution(mesh):
    both = ("plane", "tile")
    return jax.shard_map(
        local,
        mesh=mesh,
        in_specs=(P(None, both), P(both, None), P(both), P(), P("plane")),
        out_specs=P("plane", "tile"),
        check_vma=False,
    )
```

```python
import math

import jax
import jax.numpy as jnp
from jax import lax
from jax.experimental import pallas as pl
from jax.experimental.pallas import tpu as pltpu
from jax.sharding import PartitionSpec as P


G = 4096
KS = 8
CHUNKS, SUB = 8, 2
MESH = pl.DeviceIdType.MESH
F32 = jnp.float32
BF16 = jnp.bfloat16
NT = (((1,), (1,)), ((), ()))

SIN = (3.1415927410125732, -5.167710304260254, 2.550077438354492, -0.598291277885437, 0.07765766233205795)
COS = (0.9999999403953552, -4.934792995452881, 4.058411121368408, -1.331876516342163, 0.21968960762023926)


def poly(coefs, g):
    out = g * coefs[-1] + coefs[-2]
    for c in coefs[-3::-1]:
        out = out * g + c
    return out


def cos_sin(cycles):
    f = cycles - jnp.floor(cycles + 0.5)
    g = f * f
    s = f * poly(SIN, g)
    c = poly(COS, g)
    s2 = s + s
    return 1.0 - s2 * s, s2 * c


def rotated(re, im, c, s):
    return re * c - im * s, re * s + im * c


def dft(re, im):
    n = len(re)
    if n == 1:
        return re, im
    er, ei = dft(re[0::2], im[0::2])
    dr, di = dft(re[1::2], im[1::2])
    h = n // 2
    out_r, out_i = [None] * n, [None] * n
    for k in range(h):
        if k == 0:
            tr, ti = dr[k], di[k]
        elif 4 * k == n:
            tr, ti = -di[k], dr[k]
        elif 8 * k == n:
            q = math.sqrt(0.5)
            tr, ti = (dr[k] - di[k]) * q, (dr[k] + di[k]) * q
        elif 8 * k == 3 * n:
            q = math.sqrt(0.5)
            tr, ti = (dr[k] + di[k]) * -q, (dr[k] - di[k]) * q
        else:
            c, s = math.cos(2 * math.pi * k / n), math.sin(2 * math.pi * k / n)
            tr, ti = dr[k] * c - di[k] * s, dr[k] * s + di[k] * c
        out_r[k], out_i[k] = er[k] + tr, ei[k] + ti
        out_r[k + h], out_i[k + h] = er[k] - tr, ei[k] - ti
    return out_r, out_i


def sort(in_ref, out_ref):
    count = in_ref.shape[1]
    blk = 256
    ii = lax.broadcasted_iota(jnp.int32, (blk, blk), 0)
    jj = lax.broadcasted_iota(jnp.int32, (blk, blk), 1)
    tri = jnp.where(ii < jj, 1.0, 0.0).astype(BF16)
    rows = lax.broadcasted_iota(jnp.int32, (128, blk), 0).astype(F32)
    ranks = lax.broadcasted_iota(jnp.int32, (32, blk), 0).astype(F32)
    carry = jnp.zeros((128, 1), F32)
    acc = jnp.zeros((128, 128), F32)
    for b in range(count // blk):
        sl = slice(b * blk, (b + 1) * blk)
        one = jnp.where(rows == in_ref[2:3, sl], 1.0, 0.0)
        oneb = one.astype(BF16)
        before = jnp.dot(oneb, tri, preferred_element_type=F32)
        rank = jnp.sum(one * (before + carry), axis=0, keepdims=True)
        carry = carry + jnp.sum(one, axis=1, keepdims=True)
        hit = ranks == rank
        off = in_ref[3:4, sl]
        high = jnp.floor(off * (1.0 / 4096.0)) * 4096.0
        mid = jnp.floor((off - high) * (1.0 / 16.0)) * 16.0
        parts = [high, mid, off - high - mid]
        left = [in_ref[0:1, sl], in_ref[1:2, sl]]
        for k in range(3):
            cols = []
            for v in range(2):
                top = left[v].astype(BF16).astype(F32)
                left[v] = left[v] - top
                cols.append(jnp.where(hit, top, 0.0))
            cols.append(jnp.where(hit, parts[k], 0.0))
            cols.append(jnp.zeros((32, blk), F32))
            table = jnp.concatenate(cols, axis=0).astype(BF16)
            acc = acc + lax.dot_general(oneb, table, NT, preferred_element_type=F32)
    for q in range(8):
        out_ref[q // 4, q % 4] = acc[q * 16 : q * 16 + 16]


def place():
    p = lax.axis_index("plane")
    t = lax.axis_index("tile")
    return p // 4, p % 4, t // 8, (t // 2) % 4, t % 2


def kernel(in_ref, out_ref, *scratch):
    sb, wb, wo, ra, ga, hs, hp, eq, dm, tw, xs, ts, rs, sr, si, pb, r1, fw, rc, zb, zr, oh = scratch[:22]
    sa, qa, sn, qn, sv, qv, sc, qc, sw, qw, s1, q1, sf, qf, sz, qz = scratch[22:]
    zh, x, zl, y, core = place()
    z = zh * 2 + zl
    p, t = zh * 4 + x, zl * 8 + y * 2 + core
    xp, xm = (x + 1) % 4, (x + 3) % 4

    def at_x(d):
        return {"plane": zh * 4 + (x + d) % 4, "tile": t}

    def at_y(d):
        return {"plane": p, "tile": zl * 8 + ((y + d) % 4) * 2 + core}

    def at_z(d):
        zz = (z + d) % 4
        return {"plane": (zz // 2) * 4 + x, "tile": (zz % 2) * 8 + y * 2 + core}

    partner = {"plane": p, "tile": zl * 8 + y * 2 + (1 - core)}
    right, left, across = at_x(1), at_x(3), at_z(2)

    barrier = pltpu.get_barrier_semaphore()
    for d in (1, 2, 3):
        for at in (at_x, at_y, at_z):
            pl.semaphore_signal(barrier, inc=1, device_id=at(d), device_id_type=MESH)
    pl.semaphore_signal(barrier, inc=1, device_id=partner, device_id_type=MESH)

    def copy(src, dst, send, recv, device):
        return pltpu.make_async_remote_copy(
            src_ref=src, dst_ref=dst, send_sem=send, recv_sem=recv, device_id=device, device_id_type=MESH
        )

    for q in range(8):
        a = lax.broadcasted_iota(jnp.int32, (32, 256), 0) + q * 32
        b = lax.broadcasted_iota(jnp.int32, (32, 256), 1)
        c, s = cos_sin(((a * b) % 256).astype(F32) * (1.0 / 256.0))
        dm[q * 32 : q * 32 + 32] = c.astype(BF16)
        dm[256 + q * 32 : 288 + q * 32] = s.astype(BF16)
    a = lax.broadcasted_iota(jnp.int32, (16, 256), 0)
    b = lax.broadcasted_iota(jnp.int32, (16, 256), 1)
    c, s = cos_sin((a * b).astype(F32) * (1.0 / G))
    tw[0] = c
    tw[1] = s
    sort(in_ref, sb)
    small = in_ref[4:5, 0:128]

    def spread(n, shape):
        return jnp.broadcast_to(small[:, n : n + 1], shape)

    wb[...] = spread(KS, (8, 128))
    wo[zh] = wb[...]
    pl.semaphore_wait(barrier, 10)
    first = [copy(sb.at[:, (x + d) % 4], ra.at[x], sa.at[d - 1], qa.at[d - 1], at_x(d)) for d in (1, 3, 2)]
    for c in first:
        c.start()
    wcopy = copy(wb, wo.at[zh], sw, qw, across)
    wcopy.start()
    ra[x] = sb[:, x]

    l0 = lax.broadcasted_iota(jnp.int32, (256, 128), 0)
    lane = lax.broadcasted_iota(jnp.int32, (256, 128), 1)
    ec, es = cos_sin((l0 * 16 + lane).astype(F32) * (1.0 / G))
    ar, ai = spread(KS - 1, (256, 128)), jnp.zeros((256, 128), F32)
    for j in range(KS - 2, -1, -1):
        ar, ai = rotated(ar, ai, ec, es)
        ar = ar + spread(j, (256, 128))
    sr[...] = ar
    si[...] = ai
    m = t * 256 + zh * 128 + lax.broadcasted_iota(jnp.int32, (8, 128), 1)
    ec, es = cos_sin(m.astype(F32) * (1.0 / G))
    taps_low = [spread(j, (8, 128)).astype(BF16).astype(F32) for j in range(KS)]
    tr, ti = taps_low[KS - 1], jnp.zeros((8, 128), F32)
    for j in range(KS - 2, -1, -1):
        tr, ti = rotated(tr, ti, ec, es)
        tr = tr + taps_low[j]
    tr, ti = tr[0:1] * (1.0 / 512.0), ti[0:1] * (1.0 / 512.0)
    ym = jnp.where(m >= G // 2, m - G, m).astype(F32)[0:1] * (0.5 / G)
    ysq = ym * ym
    row64 = lax.broadcasted_iota(jnp.int32, (64, 128), 0)
    lane64 = lax.broadcasted_iota(jnp.int32, (64, 128), 1)

    def screen(n, _):
        v = jnp.where(n < 16, zh, 1 - zh)
        i = n % 16
        w = wo[v, 0:1, :]
        for q in range(4):
            rows = slice(q * 64, q * 64 + 64)
            l = (row64 + q * 64) * 16 + i
            xl = jnp.where(l >= G // 2, l - G, l).astype(F32) * (0.5 / G)
            rho = xl * xl + ysq
            n_minus = -rho / (1.0 + jnp.sqrt(1.0 - rho))
            c, s = cos_sin(w * n_minus)
            c, s = rotated(c, s, tr, ti)
            cs = jnp.sum(jnp.where(lane64 == i, sr[rows], 0.0), axis=1, keepdims=True)
            ss = jnp.sum(jnp.where(lane64 == i, si[rows], 0.0), axis=1, keepdims=True)
            c, s = rotated(c, s, cs, ss)
            eq[v, i, 0, rows] = c
            eq[v, i, 1, rows] = s
        return 0

    lax.fori_loop(0, 13, screen, 0)
    for c in first:
        c.wait()

    outer, inner = (z, y), (y, z)
    around = ((at_y, at_z), (at_z, at_y))

    def rows_of(h, g, cr):
        step = jnp.where(g == 0, 0, jnp.where(g == 1, 3, g - 1))
        o = (outer[h] + step) % 4
        return ga.at[pl.ds(pl.multiple_of(h * 1536 + (o * 2 + cr) * 192, 192), 192)]

    got = [ra[s].reshape(32, 128) for s in range(4)]
    group = lax.broadcasted_iota(jnp.int32, (32, 128), 1) // 32
    base = [pl.multiple_of(h * 1536 + ((outer[h] * 2 + core) * 4 + inner[h]) * 48, 48) for h in range(2)]
    for k in range(3):
        row = jnp.zeros((32, 128), F32)
        for s in range(4):
            shift = (32 * (s - k)) % 128
            moved = pltpu.roll(got[s], shift, 1) if shift else got[s]
            row = jnp.where(group == s, moved, row)
        for h in range(2):
            ga[pl.ds(base[h] + k * 16, 16)] = row[h * 16 : h * 16 + 16]
    near = []
    for d in (1, 3, 2):
        for h in range(2):
            mine = ga.at[pl.ds(base[h], 48)]
            near.append(copy(mine, mine, sn.at[h, d - 1], qn.at[h, d - 1], around[h][0](d)))
    for c in near:
        c.start()
    wcopy.wait()
    lax.fori_loop(13, 28, screen, 0)
    for c in near:
        c.wait()

    far = []
    for g, d in ((1, 1), (2, 3), (3, 2)):
        for h in range(2):
            own = rows_of(h, 0, core)
            far.append(copy(own, own, sv.at[h, g], qv.at[h, g], around[h][1](d)))

    def arrival(h, g):
        part = rows_of(h, g, core)
        return copy(part, part, sv.at[h, g], qv.at[h, g], across)

    def swap(h, g):
        part = rows_of(h, g, core)
        return copy(part, part, sc.at[h, g], qc.at[h, g], partner)

    def swapped(h, g):
        part = rows_of(h, g, 1 - core)
        return copy(part, part, sc.at[h, g], qc.at[h, g], partner)

    for h in range(2):
        swap(h, 0).start()
    for c in far:
        c.start()

    mb = (t * 256 + zh * 128).astype(F32)
    sub = lax.broadcasted_iota(jnp.int32, (8, 128), 0).astype(F32)

    def start_of(h, g):
        step = jnp.where(g == 0, 0, jnp.where(g == 1, 3, g - 1))
        o = (jnp.where(h == 0, outer[0], outer[1]) + step) % 4
        return h * 1536 + o * 384

    def dense(start, u):
        re = ga[pl.ds(start, 8, stride=48), :]
        im = ga[pl.ds(start + 16, 8, stride=48), :]
        off = ga[pl.ds(start + 32, 8, stride=48), :]
        row = jnp.floor(off * (1.0 / G))
        col = off - row * G
        cb, sb_ = cos_sin(col * mb * (1.0 / G))
        c1, s1_ = cos_sin(col * (1.0 / G))
        c8, s8 = cos_sin(col * (8.0 / G))
        re, im = rotated(re, im, cb, sb_)
        for s in range(8):
            nr, ni = rotated(re, im, c8, s8)
            xs[u, 0, s * 8 : s * 8 + 8] = re
            xs[u, 1, s * 8 : s * 8 + 8] = im
            xs[u, 2, s * 8 : s * 8 + 8] = nr
            xs[u, 3, s * 8 : s * 8 + 8] = ni
            if s < 7:
                re, im = rotated(re, im, c1, s1_)
        ts[u] = c8 + c8
        rs[u] = row

    def product(u):
        tabs, hots = [], []
        for dev in range(8):
            turn = jnp.broadcast_to(ts[u, dev : dev + 1, :], (8, 128))
            rows = []
            for v in range(2):
                a = xs[u, v, pl.ds(dev, 8, stride=8), :]
                b = xs[u, 2 + v, pl.ds(dev, 8, stride=8), :]
                for k in range(16):
                    rows.append(a)
                    a, b = b, turn * b - a
            tabs.append(jnp.concatenate(rows, axis=0))
            r = jnp.broadcast_to(rs[u, dev : dev + 1, :], (8, 128)) - sub
            hots.append(jnp.concatenate([jnp.where(r == 8.0 * j, 1.0, 0.0) for j in range(32)], axis=0))
        return tabs, hots

    def total(us):
        tabs, hots = [], []
        for u in us:
            a, b = product(u)
            tabs += a
            hots += b
        tab, hot = jnp.concatenate(tabs, axis=1), jnp.concatenate(hots, axis=1)
        return lax.dot_general(tab, hot, NT, preferred_element_type=F32)

    def fill(h, g, it):
        for u in range(4):
            dense(start_of(h, g) + it * 4 + u, u)

    def early(n, _):
        h, it = n // 4, n % 4
        fill(h, 0, it)
        for u in range(4):
            hs[h, it * 4 + u] = total([u])
        return 0

    for h in range(2):
        swapped(h, 0).wait_recv()
    lax.fori_loop(0, 8, early, 0)
    for h in range(2):
        arrival(h, 1).wait_recv()
        swap(h, 1).start()
    lax.fori_loop(28, 32, screen, 0)

    def late(n, _):
        g, h, it = 1 + n // 8, n // 4 % 2, n % 4

        @pl.when(n % 8 == 0)
        def _():
            for k in range(2):
                swapped(k, g).wait_recv()

        @pl.when(n == 3)
        def _():
            for f in (2, 3):
                for k in range(2):
                    arrival(k, f).wait_recv()
                    swap(k, f).start()

        fill(h, g, it)
        for u in range(4):
            hs[h, it * 4 + u] += total([u])
        return 0

    lax.fori_loop(0, 24, late, 0)

    def strip(rho):
        def some(i, _):
            v = i // 8
            m = pl.multiple_of(i % 8 * 16, 16)
            for h in range(2):
                lanes = slice(h * 128, h * 128 + 128)
                outs_r, outs_i = [], []
                for b in range(4):
                    r = [hs[v, b + 4 * k, pl.ds(m, 16), lanes] for k in range(4)]
                    q = [hs[v, b + 4 * k, pl.ds(m + 128, 16), lanes] for k in range(4)]
                    if rho % 2 == 0:
                        er, ei, dr, di = r[0] + r[2], q[0] + q[2], r[1] + r[3], q[1] + q[3]
                        yr, yi = (er + dr, ei + di) if rho == 0 else (er - dr, ei - di)
                    else:
                        er, ei, dr, di = r[0] - r[2], q[0] - q[2], r[1] - r[3], q[1] - q[3]
                        yr, yi = (er - di, ei + dr) if rho == 1 else (er + di, ei - dr)
                    if b and rho:
                        turn = 2 * math.pi * b * rho / 16
                        yr, yi = rotated(yr, yi, math.cos(turn), math.sin(turn))
                    outs_r.append(yr)
                    outs_i.append(yi)
                outs_r, outs_i = dft(outs_r, outs_i)
                for k in range(4):
                    c, d, j = outs_r[k], outs_i[k], rho + 4 * k
                    if j:
                        c, d = rotated(c, d, tw[0, j : j + 1, lanes], tw[1, j : j + 1, lanes])
                    hp[v, j, pl.ds(m, 16), lanes] = c.astype(BF16)
                    hp[v, j, pl.ds(m + 128, 16), lanes] = d.astype(BF16)
            return 0

        return some

    def row_class(i, k):
        return i // 2 + 4 * (i % 2 * 2 + k)

    def step_one(i):
        xo = (x + 2) % 4
        return (
            copy(pb.at[i, 0, xo], r1.at[i, 0], s1, q1.at[i, 0], right),
            copy(pb.at[i, 1, xo], r1.at[i, 1], s1, q1.at[i, 1], left),
        )

    def step_two(i):
        return (
            copy(fw.at[i, 0], rc.at[i, 0], sf, qf.at[i, 0], right),
            copy(fw.at[i, 1], rc.at[i, 1], sf, qf.at[i, 1], left),
        )

    def over(i):
        return copy(zb.at[i], zr.at[i], sz, qz.at[i], across)

    def compute(i):
        for k in range(SUB):
            j = row_class(i, k)
            pair = [lax.dot_general(dm[...], hp[v, j], NT, preferred_element_type=F32) for v in range(2)]
            for q in range(8):
                rows = slice(q * 32, q * 32 + 32)
                part = None
                for v in range(2):
                    pc, ps = pair[v][q * 32 : q * 32 + 32], pair[v][256 + q * 32 : 288 + q * 32]
                    dre = pc[:, :128] - ps[:, 128:]
                    dim = ps[:, :128] + pc[:, 128:]
                    term = eq[v, j, 0, rows] * dre - eq[v, j, 1, rows] * dim
                    part = term if part is None else part + term
                pb[i, q // 4, q % 4, k] = part

    def put(i, half, value):
        for k in range(SUB):
            oh[pl.ds(half * 512 + row_class(i, k), 32, stride=16), :] = value[k]

    lag1, lag2, lag3 = 2, 5, 7

    def turn(i, _):
        for rho in range(4):

            @pl.when(i == 2 * rho)
            def _():
                lax.fori_loop(0, 16, strip(rho), 0)

        @pl.when(i < CHUNKS)
        def _():
            compute(i)
            for c in step_one(i):
                c.start()

        @pl.when(jnp.logical_and(i >= lag2, i < CHUNKS + lag2))
        def _():
            j = i - lag2
            for c in step_two(j):
                c.wait_recv()
            zb[j] = pb[j, 1 - zh, x] + rc[j, 0, 1 - zh] + rc[j, 1, 1 - zh]
            over(j).start()
            put(j, zh, pb[j, zh, x] + rc[j, 0, zh] + rc[j, 1, zh])

        @pl.when(jnp.logical_and(i >= lag1, i < CHUNKS + lag1))
        def _():
            j = i - lag1
            for c in step_one(j):
                c.wait_recv()
            fw[j, 0, 0] = r1[j, 0] + pb[j, 0, xp]
            fw[j, 0, 1] = pb[j, 1, xp]
            fw[j, 1, 0] = pb[j, 0, xm]
            fw[j, 1, 1] = r1[j, 1] + pb[j, 1, xm]
            for c in step_two(j):
                c.start()

        @pl.when(i >= lag3)
        def _():
            j = i - lag3
            over(j).wait_recv()
            put(j, 1 - zh, zr[j])

        return 0

    lax.fori_loop(0, CHUNKS + lag3, turn, 0)
    out_ref[:, :128] = oh[:512]
    out_ref[:, 128:] = oh[512:]
    copy(r1, r1, s1, q1.at[0, 0], right).wait_send()
    copy(fw, fw, sf, qf.at[0, 0], right).wait_send()
    copy(zb, zb, sz, qz.at[0], right).wait_send()
    for c in far:
        c.wait_send()
    for h in range(2):
        for g in range(4):
            swap(h, g).wait_send()


def local(visibility, target, offset, taps, w_plane):
    count = visibility.shape[1]
    dma = pltpu.SemaphoreType.DMA
    vmem = pl.BlockSpec(memory_space=pltpu.VMEM)
    small = jnp.concatenate([taps, w_plane, jnp.zeros((count - KS - 1,), F32)])
    rows = [visibility, target.reshape(1, count).astype(F32), offset.reshape(1, count).astype(F32)]
    packed = jnp.concatenate(rows + [small.reshape(1, count), jnp.zeros((3, count), F32)], axis=0)
    pair = pltpu.VMEM((CHUNKS, 2, 2, SUB, 32, 128), F32)
    part = pltpu.VMEM((CHUNKS, SUB, 32, 128), F32)
    return pl.pallas_call(
        kernel,
        out_shape=jax.ShapeDtypeStruct((512, 256), F32),
        in_specs=[vmem],
        out_specs=vmem,
        scratch_shapes=[
            pltpu.VMEM((2, 4, 16, 128), F32),
            pltpu.VMEM((8, 128), F32),
            pltpu.VMEM((2, 8, 128), F32),
            pltpu.VMEM((4, 2, 16, 128), F32),
            pltpu.VMEM((3072, 128), F32),
            pltpu.VMEM((2, 16, 256, 256), F32),
            pltpu.VMEM((2, 16, 256, 256), BF16),
            pltpu.VMEM((2, 16, 2, 256, 128), F32),
            pltpu.VMEM((512, 256), BF16),
            pltpu.VMEM((2, 16, 256), F32),
            pltpu.VMEM((4, 4, 64, 128), F32),
            pltpu.VMEM((4, 8, 128), F32),
            pltpu.VMEM((4, 8, 128), F32),
            pltpu.VMEM((256, 128), F32),
            pltpu.VMEM((256, 128), F32),
            pltpu.VMEM((CHUNKS, 2, 4, SUB, 32, 128), F32),
            pltpu.VMEM((CHUNKS, 2, SUB, 32, 128), F32),
            pair,
            pair,
            part,
            part,
            pltpu.VMEM((1024, 128), F32),
        ]
        + [dma((3,))] * 2
        + [dma((2, 3))] * 2
        + [dma((2, 4))] * 4
        + [dma] * 3
        + [dma((CHUNKS, 2)), dma] * 2
        + [dma((CHUNKS,))],
        compiler_params=pltpu.CompilerParams(collective_id=0, has_side_effects=True, vmem_limit_bytes=36 << 20),
        name="dirtyimage",
    )(packed)


def solution(mesh):
    both = ("plane", "tile")
    return jax.shard_map(
        local,
        mesh=mesh,
        in_specs=(P(None, both), P(both, None), P(both), P(), P("plane")),
        out_specs=P("plane", "tile"),
        check_vma=False,
    )
```
